32 devices in a mesh: frag: 8 (over z, y), blk: 4 (over x, core).
Axes of the slice: x: 2, y: 2, z: 4, core: 2. Of those that a mesh axis runs over, the one named last changes fastest.
Arguments:
- amps: float32 [8, 128, 8, 128], P('frag', 'blk'), may hold values from -1.5 to 1.5
- exch: float32 [8, 128, 8, 128], P('frag', 'blk'), may hold values from -4 to 4
- factors: bfloat16 [8, 384, 128, 128], P('frag', 'blk'), may hold values from -0.109375 to 0.109375
- occupied_pair_ladder: float32 [8, 8, 8], P('frag'), may hold values from -1 to 1
- virtual_fock_block: float32 [8, 128, 128], P('frag'), may hold values from -0.1875 to 0.1875
- virtual_orbital_energy: float32 [8, 128], P('frag'), may hold values from 1 to 3
- pair_energy: float32 [8, 8], P('frag'), may hold values from -1.5 to -0.5
- energy_weight: int32 [8, 8], P('frag'), may hold values from 0 to 2
- export_rows: int32 [8, 2, 2], P('frag'), may hold values from 2 to 5, as said below
Outputs:
- new_amps: float32 [8, 128, 8, 128], P('frag', 'blk')
- res_norms: float32 [8, 2], P('frag')
- energy: float32 [], replicated
The draws below stay inside these ranges and needn't reach their ends.
Inputs may be any that keep to these rules, and one draw needn't show every extreme that they name: `export_rows`: for each fragment the 4 entries are distinct core rows.
All inputs are finite; a program needn't handle non-finite values.
Results may differ from the reference program's by a relative error of at most 0.0009.
Values may be sent and summed in bfloat16 or wider, within the bound.
A program may use at most 128 MiB of HBM per device.

```python
import math
import jax
import jax.numpy as jnp
from jax import lax

V = 128
NAUX = 384
P_SIZE = 8
BUF = 2
PASSES = 2
FRAGS = 8


def fragment_rows(key):
    chosen = jax.random.permutation(key, P_SIZE - 2 * BUF)[:2 * BUF]
    return (chosen + BUF).astype(jnp.int32).reshape(2, BUF)


def draw_export_rows(key, part):
    keys = jax.random.split(jax.random.fold_in(key, 17), FRAGS)
    return jax.vmap(fragment_rows)(keys)


def with_ends(drawn, stream_key, smallest, largest):
    dims = drawn.shape
    index_at = [jax.random.randint(jax.random.fold_in(stream_key, axis), (), 0, dims[axis]) for axis in range(len(dims))]
    drawn = drawn.at[tuple(index_at)].set(smallest)
    longest = dims.index(max(dims))
    index_at[longest] = (index_at[longest] + 1) % dims[longest]
    return drawn.at[tuple(index_at)].set(largest)


def level_of(stream_key, dims, cuts, least, high):
    factor_of, own = 1.0, jax.random.fold_in(stream_key, 6)
    for axis_at, blocks in cuts:
        heights = jnp.exp(jax.random.uniform(jax.random.fold_in(own, axis_at), (blocks,), jnp.float32, least / len(cuts), high / len(cuts)))
        factor_of = factor_of * jnp.repeat(heights, dims[axis_at] // blocks).reshape([-1 if axis == axis_at else 1 for axis in range(len(dims))])
    return factor_of


def normal_values(stream_key, extent, deviation, reach, cuts=(), kind=jnp.bfloat16):
    level = level_of(stream_key, extent, cuts, -0.22, 0.18) if cuts else 1.0
    entries = jax.random.normal(stream_key, extent, jnp.float32) * deviation * level
    return jnp.minimum(jnp.maximum(entries, -reach), reach).astype(kind)


def setup_inputs(seed: int = 0) -> dict:
    streams_of = jax.random.split(jax.random.key(seed), 10)
    amps = normal_values(streams_of[0], (FRAGS, V, P_SIZE, V), 0.1, 1.5, ((0, 8), (1, 4)), jnp.float32)
    exch = normal_values(streams_of[1], (FRAGS, V, P_SIZE, V), 0.3, 4.0, ((0, 8), (1, 4)), jnp.float32)
    factors = normal_values(streams_of[2], (FRAGS, NAUX, V, V), (V * NAUX // 16) ** -0.5, 0.109375, ((0, 8), (1, 4)))
    occupied_pair_ladder = normal_values(streams_of[3], (FRAGS, P_SIZE, P_SIZE), (4 * P_SIZE) ** -0.5, 1.0, ((0, 8),), jnp.float32)
    virtual_fock_block = normal_values(streams_of[4], (FRAGS, V, V), (8 * V) ** -0.5, 0.1875, ((0, 8),), jnp.float32)
    virtual_orbital_energy = jnp.clip(1.0 + 2.0 * jax.random.uniform(streams_of[5], (FRAGS, V), jnp.float32) ** level_of(streams_of[5], (FRAGS, V), ((0, 8),), -0.2, 0.2), 1.0, 3.0)
    pair_energy = jnp.clip(-1.5 + 1.0 * jax.random.uniform(streams_of[6], (FRAGS, P_SIZE), jnp.float32) ** level_of(streams_of[6], (FRAGS, P_SIZE), ((0, 8),), -0.2, 0.2), -1.5, -0.5)
    energy_weight = with_ends(jax.random.randint(streams_of[7], (FRAGS, P_SIZE), 0, 3), jax.random.fold_in(streams_of[7], 1), 0, 2).astype(jnp.int32)
    export_rows = draw_export_rows(jax.random.fold_in(streams_of[9], 71), 0)
    return dict(amps=amps, exch=exch, factors=factors, occupied_pair_ladder=occupied_pair_ladder, virtual_fock_block=virtual_fock_block, virtual_orbital_energy=virtual_orbital_energy, pair_energy=pair_energy, energy_weight=energy_weight, export_rows=export_rows)


def ladder_term(factor_whole, cluster_amplitude):
    block_size = math.gcd(NAUX, 48)
    low_amps = lax.optimization_barrier(cluster_amplitude.astype(jnp.bfloat16)).astype(jnp.float32)
    flat_amps = low_amps.reshape(V, P_SIZE * V)
    total = jnp.zeros((V, P_SIZE, V), jnp.float32)
    for block_index in range(NAUX // block_size):
        lower_edge = block_index * block_size
        factor_block = factor_whole[lower_edge:lower_edge + block_size]
        half_done = jnp.dot(factor_block.reshape(block_size * V, V), flat_amps, preferred_element_type=jnp.float32, precision=lax.Precision.HIGHEST)
        half_done = lax.optimization_barrier(half_done.astype(jnp.bfloat16)).astype(jnp.float32)
        half_done = half_done.reshape(block_size, V, P_SIZE, V)
        total = total + jnp.einsum('qapd,qbd->apb', half_done, factor_block, precision=lax.Precision.HIGHEST)
    return total

def one_fragment(inputs):
    amps, exch, factors, occupied_pair_ladder, virtual_fock_block, virtual_orbital_energy, pair_energy = inputs
    factor_whole = factors.astype(jnp.float32)
    denominator = virtual_orbital_energy[:, None, None] + virtual_orbital_energy[None, None, :] - pair_energy[None, :, None]
    cluster_amplitude = amps
    norms = []
    for sweep_index in range(PASSES):
        ladder = ladder_term(factor_whole, cluster_amplitude)
        hole = jnp.einsum('pr,arb->apb', occupied_pair_ladder, cluster_amplitude, precision=lax.Precision.HIGHEST)
        fock_section = jnp.einsum('vn,nog->vog', virtual_fock_block, cluster_amplitude, precision=lax.Precision.HIGHEST)
        fock_section = fock_section + jnp.einsum('apc,bc->apb', cluster_amplitude, virtual_fock_block, precision=lax.Precision.HIGHEST)
        residual = exch + ladder + hole + fock_section - denominator * cluster_amplitude
        norms.append(jnp.sqrt(jnp.sum(residual * residual)))
        cluster_amplitude = cluster_amplitude + residual / denominator
    return (cluster_amplitude, jnp.stack(norms))

def pick_rows(cluster_amplitude, picked):
    return jnp.take(cluster_amplitude, picked, axis=1)

def reference(amps, exch, factors, occupied_pair_ladder, virtual_fock_block, virtual_orbital_energy, pair_energy, energy_weight, export_rows):
    all_amps, res_norms = lax.map(one_fragment, (amps, exch, factors, occupied_pair_ladder, virtual_fock_block, virtual_orbital_energy, pair_energy))
    upward = jax.vmap(pick_rows)(all_amps, export_rows[:, 0, :])
    downward = jax.vmap(pick_rows)(all_amps, export_rows[:, 1, :])
    lower = jnp.concatenate([all_amps[:1, :, :BUF], upward[:-1]], axis=0)
    upper = jnp.concatenate([downward[1:], all_amps[-1:, :, P_SIZE - BUF:]], axis=0)
    new_amps = jnp.concatenate([lower, all_amps[:, :, BUF:P_SIZE - BUF], upper], axis=2)
    weights = energy_weight.astype(jnp.float32) * 0.5
    energy = -jnp.sum(weights[:, None, :, None] * new_amps * exch) / (V * V)
    return (new_amps, res_norms, energy)
```

```python
import functools

import jax
import jax.numpy as jnp
from jax import lax
from jax.experimental import pallas as pl
from jax.experimental.pallas import tpu as pltpu
from jax.sharding import PartitionSpec as P

PASSES = 2
CHUNK = 2
UNITS = 2
GROUP = 8
MESH = pl.DeviceIdType.MESH
F32, BF16 = jnp.float32, jnp.bfloat16


def halves(value):
    high = value.astype(BF16)
    return high, (value - high.astype(F32)).astype(BF16)


def kernel(blocks, frags, *refs):
    virt = refs[0].shape[3]
    tall, flat = (2 * virt, 2 * virt), (virt, 2 * virt)

    def body(first, ladder, left, right):
        run(blocks, frags, first, ladder, left, right, *refs)

    pl.run_scoped(
        body,
        [[pltpu.ACC(m)(tall, F32) for _ in range(2)] for m in range(UNITS)],
        [[pltpu.ACC(m)(flat, F32) for _ in range(2)] for m in range(UNITS)],
        [pltpu.ACC(m)(flat, F32) for m in range(UNITS)],
        [pltpu.ACC(m)(flat, F32) for m in range(UNITS)],
    )


def run(
    blocks,
    frags,
    first_acc,
    ladder_acc,
    left_acc,
    right_acc,
    amps_hbm,
    exch_hbm,
    factors_hbm,
    hole_hbm,
    fock_hbm,
    orbital_hbm,
    pair_hbm,
    weight_hbm,
    export_hbm,
    new_ref,
    norm_ref,
    energy_ref,
    fact,
    amps_in,
    exch_in,
    fock_in,
    orbital_in,
    hole_ref,
    pair_ref,
    weight_ref,
    export_ref,
    amp,
    low,
    half,
    part,
    recv,
    base,
    recip,
    fock_row,
    fock_col,
    row_energy,
    row_t,
    sent_rows,
    got_rows,
    sums,
    in_sem,
    fact_sem,
    ag_send,
    ag_recv,
    rs_send,
    rs_recv,
    ex_send,
    ex_recv,
    sum_send,
    sum_recv,
):
    me = lax.axis_index("blk")
    frag = lax.axis_index("frag")
    rows, pairs, virt = amps_in.shape
    aux = fact.shape[0]
    groups = aux // GROUP
    border = export_hbm.shape[2]
    devices = blocks * frags
    device = frag * blocks + me
    peers = [lax.rem(me + j, blocks) for j in range(1, blocks)]
    starts = sorted(
        range(0, pairs, CHUNK), key=lambda p: p < border or p + CHUNK > pairs - border
    )
    chunks = len(starts)
    core_chunks = sum(1 for p in starts if border <= p and p + CHUNK <= pairs - border)
    turns = PASSES * chunks
    count = turns * groups

    def place(turn):
        return turn // chunks, starts[turn % chunks]

    def other(j):
        there = lax.rem(device + j, devices)
        return {"frag": there // blocks, "blk": lax.rem(there, blocks)}

    loads = []
    for i, (src, dst) in enumerate(
        (
            (amps_hbm.at[0], amps_in),
            (fock_hbm.at[0], fock_in),
            (orbital_hbm, orbital_in),
            (pair_hbm, pair_ref),
            (hole_hbm, hole_ref),
            (exch_hbm.at[0], exch_in),
            (weight_hbm, weight_ref),
            (export_hbm, export_ref),
        )
    ):
        loads.append(pltpu.make_async_copy(src, dst, in_sem.at[i]))
    fact_loads = [
        pltpu.make_async_copy(
            factors_hbm.at[0, pl.ds(g * GROUP, GROUP)],
            fact.at[pl.ds(g * GROUP, GROUP)],
            fact_sem.at[g],
        )
        for g in range(groups)
    ]
    for copy in loads[:6]:
        copy.start()
    for copy in fact_loads:
        copy.start()
    for copy in loads[6:]:
        copy.start()

    barrier = pltpu.get_barrier_semaphore()

    def greet(j, carry):
        pl.semaphore_signal(barrier, inc=1, device_id=other(j), device_id_type=MESH)
        return carry

    lax.fori_loop(1, devices, greet, 0)

    for m in range(UNITS):
        for ref in first_acc[m] + ladder_acc[m] + [left_acc[m], right_acc[m]]:
            pltpu.matmul_pop(ref)

    loads[0].wait()
    for p in range(pairs):
        value = amps_in[:, p, :]
        amp[0, p] = value
        low[0, me, p] = value.astype(BF16)
    pl.semaphore_wait(barrier, devices - 1)

    pending = []

    def gather(turn):
        sweep, start = place(turn)
        copies = []
        for j, peer in enumerate(peers):
            where = low.at[sweep, me, pl.ds(start, CHUNK)]
            copy = pltpu.make_async_remote_copy(
                src_ref=where,
                dst_ref=where,
                send_sem=ag_send.at[turn, j],
                recv_sem=ag_recv.at[turn, j],
                device_id={"blk": peer},
                device_id_type=MESH,
            )
            copy.start()
            copies.append(copy)
        pending.extend(copies)
        return copies

    gathers = {turn: gather(turn) for turn in range(chunks)}

    def scatter(turn):
        copies = []
        for j, peer in enumerate(peers):
            copy = pltpu.make_async_remote_copy(
                src_ref=part.at[turn, peer],
                dst_ref=recv.at[turn, j],
                send_sem=rs_send.at[turn, j],
                recv_sem=rs_recv.at[turn, j],
                device_id={"blk": peer},
                device_id_type=MESH,
            )
            copy.start()
            copies.append(copy)
        pending.extend(copies)
        return copies

    offset = pl.multiple_of(me * rows, rows)
    for copy in loads[1:5]:
        copy.wait()
    column = lax.broadcasted_iota(jnp.int32, (virt, virt), 1)
    own = (column >= offset) & (column < offset + rows)
    high, middle = halves(fock_in[...])
    fock_row[:, :virt] = high
    fock_row[:, virt:] = middle
    high, middle = halves(jnp.where(own, fock_in[...], 0.0))
    fock_col[:, :virt] = high
    fock_col[:, virt:] = middle
    row_t[...] = jnp.broadcast_to(orbital_in[...], (virt, virt)).T
    row_energy[...] = row_t[pl.ds(offset, rows), :] + orbital_in[...]
    for p in range(pairs):
        recip[p] = 1.0 / (row_energy[...] - pair_ref[0, p])
    loads[5].wait()

    def make_base(sweep, register):
        share = pairs // UNITS
        tile = jnp.concatenate([fock_row[...], jnp.zeros((virt, 2 * virt), BF16)], axis=0)
        for m in range(UNITS):
            pltpu.matmul_push_rhs(tile, staging_register=register, mxu_index=m, transpose=True)
        for m in range(UNITS):
            split = halves(amp[sweep, m * share : (m + 1) * share].reshape(share * rows, virt))
            for i, value in enumerate(split):
                pltpu.matmul_acc_lhs(
                    right_acc[m],
                    jnp.concatenate([value, value], axis=1),
                    load_staged_rhs=register if i == 0 else None,
                )
        for m in range(UNITS):
            product = pltpu.matmul_pop(right_acc[m])
            for k in range(share):
                p = m * share + k
                total = exch_in[:, p, :] + product[k * rows : (k + 1) * rows, :virt]
                for r in range(pairs):
                    total = total + hole_ref[0, p, r] * amp[sweep, r]
                total = total - (row_energy[...] - pair_ref[0, p]) * amp[sweep, p]
                base[sweep, p] = total

    make_base(0, 0)

    def add_left(turn, register):
        sweep, start = place(turn)
        split = [halves(amp[sweep, start + i]) for i in range(CHUNK)]
        for m in range(UNITS):
            tile = jnp.concatenate([split[i][m] for i in range(CHUNK)], axis=1)
            tile = jnp.concatenate([tile] * (2 * blocks), axis=0)
            pltpu.matmul_push_rhs(tile, staging_register=register, mxu_index=m)
            pltpu.matmul_acc_lhs(left_acc[m], fock_col[...], load_staged_rhs=register)

    def aux_at(step, m, i):
        return (step % groups) * GROUP + m * (GROUP // UNITS) + 2 * i

    def push_amp(step, register):
        turn = step // groups
        sweep, start = place(turn)
        if step % groups == 0:
            for copy in gathers[turn]:
                copy.wait_recv()
        tile = jnp.concatenate(
            [low[sweep, :, start + i].reshape(virt, virt) for i in range(CHUNK)], axis=1
        )
        tile = jnp.concatenate([tile, jnp.zeros((virt, 2 * virt), BF16)], axis=0)
        for m in range(UNITS):
            pltpu.matmul_push_rhs(tile, staging_register=register, mxu_index=m)

    def first_half(step, i, register):
        if step < groups and i == 0:
            fact_loads[step].wait()
        for m in range(UNITS):
            q = aux_at(step, m, i)
            slab = fact[q : q + 2].reshape(2 * virt, virt)
            pltpu.matmul_acc_lhs(
                first_acc[m][i],
                jnp.concatenate([slab, jnp.zeros_like(slab)], axis=1),
                load_staged_rhs=register if i == 0 else None,
            )

    def turn_half(i, register):
        for m in range(UNITS):
            done = pltpu.matmul_pop(first_acc[m][i]).astype(BF16)
            for p in range(CHUNK):
                for q in range(2):
                    half[m, i, p, q] = done[q * virt : (q + 1) * virt, p * virt : (p + 1) * virt]

    def push_half(i, register):
        for m in range(UNITS):
            tile = jnp.concatenate(
                [
                    jnp.concatenate([half[m, i, p, q] for q in range(2)], axis=1)
                    for p in range(CHUNK)
                ],
                axis=0,
            )
            pltpu.matmul_push_rhs(tile, staging_register=register, mxu_index=m, transpose=True)

    def second_half(step, i, register):
        turn = step // groups
        for m in range(UNITS):
            q = aux_at(step, m, i)
            pltpu.matmul_acc_lhs(
                ladder_acc[m][turn % 2],
                jnp.concatenate([fact[q], fact[q + 1]], axis=1),
                load_staged_rhs=register,
            )

    def group(step):
        now, free = step % 2, 1 - step % 2
        more = step + 1 < count
        turn_half(0, free)
        if more:
            first_half(step + 1, 0, now)
        push_half(0, free)
        turn_half(1, now)
        if more:
            first_half(step + 1, 1, now)
        push_half(1, now)
        second_half(step, 0, free)
        if step + 2 < count:
            push_amp(step + 2, free)
        second_half(step, 1, now)

    def give(turn):
        total = pltpu.matmul_pop(ladder_acc[0][turn % 2])
        side = pltpu.matmul_pop(left_acc[0])
        for m in range(1, UNITS):
            total = total + pltpu.matmul_pop(ladder_acc[m][turn % 2])
            side = side + pltpu.matmul_pop(left_acc[m])
        for i in range(CHUNK):
            cols = slice(i * virt, (i + 1) * virt)
            value = total[:, cols].T + side[:, cols]
            for k in range(blocks):
                part[turn, k, i] = value[k * rows : (k + 1) * rows]
        return scatter(turn)

    norm_sums = [jnp.zeros((8, virt), F32) for _ in range(PASSES)]

    def finish(turn, copies):
        sweep, start = place(turn)
        for copy in copies:
            copy.wait_recv()
        for i in range(CHUNK):
            p = start + i
            residual = base[sweep, p] + part[turn, me, i]
            for j in range(blocks - 1):
                residual = residual + recv[turn, j, i]
            norm_sums[sweep] += jnp.sum((residual * residual).reshape(rows // 8, 8, virt), axis=0)
            value = amp[sweep, p] + residual * recip[p]
            amp[sweep + 1, p] = value
            if sweep + 1 < PASSES:
                low[sweep + 1, me, p] = value.astype(BF16)
        if sweep + 1 < PASSES:
            gathers[turn + chunks] = gather(turn + chunks)

    exports = []

    def export():
        for side, target in ((0, lax.rem(frag + 1, frags)), (1, lax.rem(frag + frags - 1, frags))):
            for r in range(border):
                sent_rows[side, r] = amp[PASSES, export_ref[0, side, r]]
            copy = pltpu.make_async_remote_copy(
                src_ref=sent_rows.at[side],
                dst_ref=got_rows.at[side],
                send_sem=ex_send.at[side],
                recv_sem=ex_recv.at[side],
                device_id={"frag": target},
                device_id_type=MESH,
            )
            copy.start()
            exports.append(copy)
        pending.extend(exports)

    energy = [jnp.zeros((8, virt), F32)]

    def settle(p):
        value = amp[PASSES, p]
        if p < border:
            value = jnp.where(frag > 0, got_rows[0, p], value)
        if p >= pairs - border:
            value = jnp.where(frag < frags - 1, got_rows[1, p - (pairs - border)], value)
        new_ref[0, :, p, :] = value
        product = jnp.sum((value * exch_in[:, p, :]).reshape(rows // 8, 8, virt), axis=0)
        energy[0] = energy[0] + (weight_ref[0, p].astype(F32) * 0.5) * product

    push_amp(0, 1)
    first_half(0, 0, 1)
    first_half(0, 1, 1)
    push_amp(1, 0)
    given = {}
    for turn in range(turns):
        for g in range(groups):
            step = turn * groups + g
            group(step)
            if g == 0:
                if turn > 0:
                    given[turn - 1] = give(turn - 1)
                add_left(turn, step % 2)
            if g == groups // 2 - 1 and turn >= 2:
                finish(turn - 2, given[turn - 2])
                if turn - 2 == chunks - 1:
                    make_base(1, step % 2)
                if turn - 2 == (PASSES - 1) * chunks + core_chunks - 1:
                    for copy in loads[6:]:
                        copy.wait()
                    export()
    given[turns - 1] = give(turns - 1)
    finish(turns - 2, given[turns - 2])
    late = [p for t in range(turns - 1, turns) for p in range(place(t)[1], place(t)[1] + CHUNK)]
    for copy in exports:
        copy.wait_recv()
    for p in range(pairs):
        if p not in late:
            settle(p)
    finish(turns - 1, given[turns - 1])
    for p in late:
        settle(p)

    def whole(value):
        return jnp.sum(jnp.sum(value, axis=0, keepdims=True), axis=1, keepdims=True)

    lane = lax.broadcasted_iota(jnp.int32, (1, virt), 1)
    line = jnp.where(lane == PASSES, whole(energy[0]), 0.0)
    for s in range(PASSES):
        line = jnp.where(lane == s, whole(norm_sums[s]), line)
    sums[device] = line

    def sum_copy(j):
        return pltpu.make_async_remote_copy(
            src_ref=sums.at[device],
            dst_ref=sums.at[device],
            send_sem=sum_send.at[j - 1],
            recv_sem=sum_recv.at[j - 1],
            device_id=other(j),
            device_id_type=MESH,
        )

    def send_sum(j, carry):
        sum_copy(j).start()
        return carry

    def take_sum(j, carry):
        sum_copy(j).wait_recv()
        return carry

    def sent_sum(j, carry):
        sum_copy(j).wait_send()
        return carry

    lax.fori_loop(1, devices, send_sum, 0)
    for copy in pending:
        copy.wait_send()
    lax.fori_loop(1, devices, take_sum, 0)
    norm_ref[...] = jnp.sqrt(jnp.sum(sums[pl.ds(frag * blocks, blocks)], axis=0))[:, :PASSES]
    last = jnp.where(lane == PASSES, jnp.sum(sums[...], axis=0), 0.0)
    energy_ref[...] = -jnp.sum(last, axis=1, keepdims=True) / (virt * virt)
    lax.fori_loop(1, devices, sent_sum, 0)


def on_device(blocks, frags, *args):
    amps, _, factors = args[:3]
    _, rows, pairs, virt = amps.shape
    aux = factors.shape[1]
    border = args[-1].shape[2]
    turns = PASSES * (pairs // CHUNK)
    vmem = pl.BlockSpec(memory_space=pltpu.VMEM)
    hbm = pl.BlockSpec(memory_space=pltpu.HBM)
    dma = pltpu.SemaphoreType.DMA
    new_amps, norms, energy = pl.pallas_call(
        functools.partial(kernel, blocks, frags),
        out_shape=(
            jax.ShapeDtypeStruct(amps.shape, F32),
            jax.ShapeDtypeStruct((1, PASSES), F32),
            jax.ShapeDtypeStruct((1, 1), F32),
        ),
        in_specs=[hbm] * 9,
        out_specs=(vmem, vmem, vmem),
        scratch_shapes=[
            pltpu.VMEM((aux, virt, virt), BF16),
            pltpu.VMEM((rows, pairs, virt), F32),
            pltpu.VMEM((rows, pairs, virt), F32),
            pltpu.VMEM((virt, virt), F32),
            pltpu.VMEM((1, virt), F32),
            pltpu.SMEM((1, pairs, pairs), F32),
            pltpu.SMEM((1, pairs), F32),
            pltpu.SMEM((1, pairs), jnp.int32),
            pltpu.SMEM((1, 2, border), jnp.int32),
            pltpu.VMEM((PASSES + 1, pairs, rows, virt), F32),
            pltpu.VMEM((PASSES, blocks, pairs, rows, virt), BF16),
            pltpu.VMEM((UNITS, 2, CHUNK, 2, virt, virt), BF16),
            pltpu.VMEM((turns, blocks, CHUNK, rows, virt), F32),
            pltpu.VMEM((turns, blocks - 1, CHUNK, rows, virt), F32),
            pltpu.VMEM((PASSES, pairs, rows, virt), F32),
            pltpu.VMEM((pairs, rows, virt), F32),
            pltpu.VMEM((virt, 2 * virt), BF16),
            pltpu.VMEM((virt, 2 * virt), BF16),
            pltpu.VMEM((rows, virt), F32),
            pltpu.VMEM((virt, virt), F32),
            pltpu.VMEM((2, border, rows, virt), F32),
            pltpu.VMEM((2, border, rows, virt), F32),
            pltpu.VMEM((blocks * frags, 1, virt), F32),
            dma((8,)),
            dma((aux // GROUP,)),
            dma((turns, blocks - 1)),
            dma((turns, blocks - 1)),
            dma((turns, blocks - 1)),
            dma((turns, blocks - 1)),
            dma((2,)),
            dma((2,)),
            dma((blocks * frags - 1,)),
            dma((blocks * frags - 1,)),
        ],
        compiler_params=pltpu.CompilerParams(
            collective_id=0, has_side_effects=True, vmem_limit_bytes=48 * 2**20
        ),
    )(*[pltpu.with_memory_space_constraint(x, pltpu.HBM) for x in args])
    return new_amps, norms, energy.reshape(())


def solution(mesh):
    placed = (
        P("frag", "blk", None, None),
        P("frag", "blk", None, None),
        P("frag", "blk", None, None),
        P("frag", None, None),
        P("frag", None, None),
        P("frag", None),
        P("frag", None),
        P("frag", None),
        P("frag", None, None),
    )
    return jax.shard_map(
        functools.partial(on_device, mesh.shape["blk"], mesh.shape["frag"]),
        mesh=mesh,
        in_specs=placed,
        out_specs=(P("frag", "blk", None, None), P("frag", None), P()),
        check_vma=False,
    )
```

```python
import functools

import jax
import jax.numpy as jnp
from jax import lax
from jax.experimental import pallas as pl
from jax.experimental.pallas import tpu as pltpu
from jax.sharding import PartitionSpec as P

PASSES = 2
CHUNK = 2
UNITS = 2
GROUP = 8
MESH = pl.DeviceIdType.MESH
F32, BF16 = jnp.float32, jnp.bfloat16


def halves(value):
    high = value.astype(BF16)
    return high, (value - high.astype(F32)).astype(BF16)


def kernel(blocks, frags, *refs):
    virt = refs[0].shape[3]
    tall, flat = (2 * virt, 2 * virt), (virt, 2 * virt)

    def body(first, ladder, left, right):
        run(blocks, frags, first, ladder, left, right, *refs)

    pl.run_scoped(
        body,
        [[pltpu.ACC(m)(tall, F32) for _ in range(2)] for m in range(UNITS)],
        [[pltpu.ACC(m)(flat, F32) for _ in range(2)] for m in range(UNITS)],
        [pltpu.ACC(m)(flat, F32) for m in range(UNITS)],
        [pltpu.ACC(m)(flat, F32) for m in range(UNITS)],
    )


def run(
    blocks,
    frags,
    first_acc,
    ladder_acc,
    left_acc,
    right_acc,
    amps_hbm,
    exch_hbm,
    factors_hbm,
    hole_hbm,
    fock_hbm,
    orbital_hbm,
    pair_hbm,
    weight_hbm,
    export_hbm,
    new_ref,
    norm_ref,
    energy_ref,
    fact,
    amps_in,
    exch_in,
    fock_in,
    orbital_in,
    hole_ref,
    pair_ref,
    weight_ref,
    export_ref,
    amp,
    low,
    half,
    part,
    recv,
    part_low,
    recv_low,
    exch,
    base,
    recip,
    fock_row,
    fock_col,
    row_energy,
    row_t,
    sent_rows,
    got_rows,
    sent_weights,
    got_weights,
    sums,
    squares,
    ring,
    in_sem,
    fact_sem,
    ag_send,
    ag_recv,
    rs_send,
    rs_recv,
    ex_send,
    ex_recv,
    we_send,
    we_recv,
    sum_send,
    sum_recv,
    sq_send,
    sq_recv,
):
    me = lax.axis_index("blk")
    frag = lax.axis_index("frag")
    rows, pairs, virt = amps_in.shape
    aux = fact.shape[0]
    groups = aux // GROUP
    border = export_hbm.shape[2]
    device = frag * blocks + me
    peers = [lax.rem(me + j, blocks) for j in range(1, blocks)]
    core = pairs - 2 * border
    swap = frag == frags - 1

    def pair_at(place):
        if place < core:
            return border + place
        at = (place - core) % border
        lower, upper = at, pairs - border + at
        if place - core < border:
            return jnp.where(swap, upper, lower)
        return jnp.where(swap, lower, upper)

    def take(ref, place):
        if place < core:
            return ref[:, border + place, :]
        at = (place - core) % border
        lower, upper = ref[:, at, :], ref[:, pairs - border + at, :]
        if place - core < border:
            return jnp.where(swap, upper, lower)
        return jnp.where(swap, lower, upper)

    chunks = pairs // CHUNK
    core_chunks = core // CHUNK
    turns = PASSES * chunks
    count = turns * groups

    def place(turn):
        return turn // chunks, turn % chunks * CHUNK

    sides = [lax.rem(frag + frags - 1, frags), lax.rem(frag + 1, frags)]

    loads = []
    for i, (src, dst) in enumerate(
        (
            (amps_hbm.at[0], amps_in),
            (fock_hbm.at[0], fock_in),
            (orbital_hbm, orbital_in),
            (pair_hbm, pair_ref),
            (hole_hbm, hole_ref),
            (exch_hbm.at[0], exch_in),
            (weight_hbm, weight_ref),
            (export_hbm, export_ref),
        )
    ):
        loads.append(pltpu.make_async_copy(src, dst, in_sem.at[i]))
    fact_loads = [
        pltpu.make_async_copy(
            factors_hbm.at[0, pl.ds(g * GROUP, GROUP)],
            fact.at[pl.ds(g * GROUP, GROUP)],
            fact_sem.at[g],
        )
        for g in range(groups)
    ]
    for copy in loads:
        copy.start()
    for copy in fact_loads:
        copy.start()

    barrier = pltpu.get_barrier_semaphore()

    for peer in peers:
        pl.semaphore_signal(barrier, inc=1, device_id={"blk": peer}, device_id_type=MESH)
    for side in sides:
        pl.semaphore_signal(barrier, inc=1, device_id={"frag": side}, device_id_type=MESH)

    rounds = frags // 2
    every = pl.cdiv(rounds, PASSES * chunks - 2)

    def ring_signal(r):
        for i, side in enumerate(sides):
            pl.semaphore_signal(
                ring.at[r, i], inc=1, device_id={"frag": side}, device_id_type=MESH
            )

    def ring_wait(r):
        for i in range(2):
            pl.semaphore_wait(ring.at[r, i], 1)

    for m in range(UNITS):
        for ref in first_acc[m] + ladder_acc[m] + [left_acc[m], right_acc[m]]:
            pltpu.matmul_pop(ref)

    loads[0].wait()

    def enter(place):
        value = take(amps_in, place)
        amp[0, place] = value
        low[0, me, place] = value.astype(BF16)

    for place_at in range(CHUNK):
        enter(place_at)
    pl.semaphore_wait(barrier, blocks - 1 + 2)

    pending = []

    def gather(turn):
        sweep, start = place(turn)
        copies = []
        for j, peer in enumerate(peers):
            where = low.at[sweep, me, pl.ds(start, CHUNK)]
            copy = pltpu.make_async_remote_copy(
                src_ref=where,
                dst_ref=where,
                send_sem=ag_send.at[turn, j],
                recv_sem=ag_recv.at[turn, j],
                device_id={"blk": peer},
                device_id_type=MESH,
            )
            copy.start()
            copies.append(copy)
        pending.extend(copies)
        return copies

    gathers = {0: gather(0)}
    for turn in range(1, chunks):
        for i in range(CHUNK):
            enter(turn * CHUNK + i)
        gathers[turn] = gather(turn)

    def scatter(turn):
        copies = []
        last = turn == turns - 1
        for j, peer in enumerate(peers):
            copy = pltpu.make_async_remote_copy(
                src_ref=part_low.at[peer] if last else part.at[turn, peer],
                dst_ref=recv_low.at[j] if last else recv.at[turn, j],
                send_sem=rs_send.at[turn, j],
                recv_sem=rs_recv.at[turn, j],
                device_id={"blk": peer},
                device_id_type=MESH,
            )
            copy.start()
            copies.append(copy)
        pending.extend(copies)
        return copies

    offset = pl.multiple_of(me * rows, rows)
    for copy in loads[1:5]:
        copy.wait()
    column = lax.broadcasted_iota(jnp.int32, (virt, virt), 1)
    own = (column >= offset) & (column < offset + rows)
    high, middle = halves(fock_in[...])
    fock_row[:, :virt] = high
    fock_row[:, virt:] = middle
    high, middle = halves(jnp.where(own, fock_in[...], 0.0))
    fock_col[:, :virt] = high
    fock_col[:, virt:] = middle
    row_t[...] = jnp.broadcast_to(orbital_in[...], (virt, virt)).T
    row_energy[...] = row_t[pl.ds(offset, rows), :] + orbital_in[...]
    where = [pair_at(p) for p in range(pairs)]
    levels = [pair_ref[0, p] for p in where]
    for p in range(pairs):
        recip[p] = 1.0 / (row_energy[...] - levels[p])
    for copy in loads[5:]:
        copy.wait()
    weights = [weight_ref[0, p].astype(F32) * 0.5 for p in range(pairs)]
    for p in range(pairs):
        exch[p] = take(exch_in, p)
    for i, side in enumerate(sides):
        for r in range(border):
            p = r if i == 0 else pairs - border + r
            sent_weights[i, r] = exch_in[:, p, :] * weights[p]
    weight_copies = []
    for i, side in enumerate(sides):
        copy = pltpu.make_async_remote_copy(
            src_ref=sent_weights.at[i],
            dst_ref=got_weights.at[i],
            send_sem=we_send.at[i],
            recv_sem=we_recv.at[i],
            device_id={"frag": side},
            device_id_type=MESH,
        )
        copy.start()
        weight_copies.append(copy)
    pending.extend(weight_copies)
    ring_signal(0)

    def make_base(sweep, register):
        share = pairs // UNITS
        tile = jnp.concatenate([fock_row[...], jnp.zeros((virt, 2 * virt), BF16)], axis=0)
        for m in range(UNITS):
            pltpu.matmul_push_rhs(tile, staging_register=register, mxu_index=m, transpose=True)
        for m in range(UNITS):
            split = halves(amp[sweep, m * share : (m + 1) * share].reshape(share * rows, virt))
            for i, value in enumerate(split):
                pltpu.matmul_acc_lhs(
                    right_acc[m],
                    jnp.concatenate([value, value], axis=1),
                    load_staged_rhs=register if i == 0 else None,
                )
        for m in range(UNITS):
            product = pltpu.matmul_pop(right_acc[m])
            for k in range(share):
                p = m * share + k
                total = exch[p] + product[k * rows : (k + 1) * rows, :virt]
                for r in range(pairs):
                    total = total + hole_ref[0, where[p], where[r]] * amp[sweep, r]
                total = total - (row_energy[...] - levels[p]) * amp[sweep, p]
                base[sweep, p] = total

    make_base(0, 0)

    def add_left(turn, register):
        sweep, start = place(turn)
        split = [halves(amp[sweep, start + i]) for i in range(CHUNK)]
        for m in range(UNITS):
            tile = jnp.concatenate([split[i][m] for i in range(CHUNK)], axis=1)
            tile = jnp.concatenate([tile] * (2 * blocks), axis=0)
            pltpu.matmul_push_rhs(tile, staging_register=register, mxu_index=m)
            pltpu.matmul_acc_lhs(left_acc[m], fock_col[...], load_staged_rhs=register)

    def aux_at(step, m, i):
        return (step % groups) * GROUP + m * (GROUP // UNITS) + 2 * i

    def push_amp(step, register):
        turn = step // groups
        sweep, start = place(turn)
        if step % groups == 0:
            for copy in gathers[turn]:
                copy.wait_recv()
        tile = jnp.concatenate(
            [low[sweep, :, start + i].reshape(virt, virt) for i in range(CHUNK)], axis=1
        )
        tile = jnp.concatenate([tile, jnp.zeros((virt, 2 * virt), BF16)], axis=0)
        for m in range(UNITS):
            pltpu.matmul_push_rhs(tile, staging_register=register, mxu_index=m)

    def first_half(step, i, register):
        if step < groups and i == 0:
            fact_loads[step].wait()
        for m in range(UNITS):
            q = aux_at(step, m, i)
            slab = fact[q : q + 2].reshape(2 * virt, virt)
            pltpu.matmul_acc_lhs(
                first_acc[m][i],
                jnp.concatenate([slab, jnp.zeros_like(slab)], axis=1),
                load_staged_rhs=register if i == 0 else None,
            )

    def turn_half(i, register):
        for m in range(UNITS):
            done = pltpu.matmul_pop(first_acc[m][i]).astype(BF16)
            for p in range(CHUNK):
                for q in range(2):
                    half[m, i, p, q] = done[q * virt : (q + 1) * virt, p * virt : (p + 1) * virt]

    def push_half(i, register):
        for m in range(UNITS):
            tile = jnp.concatenate(
                [
                    jnp.concatenate([half[m, i, p, q] for q in range(2)], axis=1)
                    for p in range(CHUNK)
                ],
                axis=0,
            )
            pltpu.matmul_push_rhs(tile, staging_register=register, mxu_index=m, transpose=True)

    def second_half(step, i, register):
        turn = step // groups
        for m in range(UNITS):
            q = aux_at(step, m, i)
            pltpu.matmul_acc_lhs(
                ladder_acc[m][turn % 2],
                jnp.concatenate([fact[q], fact[q + 1]], axis=1),
                load_staged_rhs=register,
            )

    def group(step):
        now, free = step % 2, 1 - step % 2
        more = step + 1 < count
        turn_half(0, free)
        if more:
            first_half(step + 1, 0, now)
        push_half(0, free)
        turn_half(1, now)
        if more:
            first_half(step + 1, 1, now)
        push_half(1, now)
        second_half(step, 0, free)
        if step + 2 < count:
            push_amp(step + 2, free)
        second_half(step, 1, now)

    def give(turn):
        total = pltpu.matmul_pop(ladder_acc[0][turn % 2])
        side = pltpu.matmul_pop(left_acc[0])
        for m in range(1, UNITS):
            total = total + pltpu.matmul_pop(ladder_acc[m][turn % 2])
            side = side + pltpu.matmul_pop(left_acc[m])
        for i in range(CHUNK):
            cols = slice(i * virt, (i + 1) * virt)
            value = total[:, cols].T + side[:, cols]
            for k in range(blocks):
                piece = value[k * rows : (k + 1) * rows]
                part[turn, k, i] = piece
                if turn == turns - 1:
                    part_low[k, i] = piece.astype(BF16)
        return scatter(turn)

    norm_sums = [jnp.zeros((8, virt), F32) for _ in range(PASSES)]
    energy = [jnp.zeros((8, virt), F32)]

    def fold(value):
        return jnp.sum(value.reshape(rows // 8, 8, virt), axis=0)

    def finish(turn, copies):
        sweep, start = place(turn)
        last = turn == turns - 1
        for copy in copies:
            copy.wait_recv()
        for i in range(CHUNK):
            p = start + i
            residual = base[sweep, p] + part[turn, me, i]
            for j in range(blocks - 1):
                residual = residual + (recv_low[j, i].astype(F32) if last else recv[turn, j, i])
            norm_sums[sweep] += fold(residual * residual)
            if last:
                continue
            value = amp[sweep, p] + residual * recip[p]
            amp[sweep + 1, p] = value
            if sweep + 1 < PASSES:
                low[sweep + 1, me, p] = value.astype(BF16)
            elif p < core:
                new_ref[:, border + p, :] = value
                energy[0] = energy[0] + weights[border + p] * fold(value * exch[p])
        if sweep + 1 < PASSES:
            gathers[turn + chunks] = gather(turn + chunks)

    exports = []

    def export():
        for copy in weight_copies:
            copy.wait_recv()
        for side, target in ((0, sides[1]), (1, sides[0])):
            used = frag < frags - 1 if side == 0 else frag > 0
            for r in range(border):
                value = amp[PASSES, jnp.maximum(export_ref[0, side, r] - border, 0)]
                sent_rows[side, r] = value
                energy[0] = energy[0] + jnp.where(used, fold(value * got_weights[side, r]), 0.0)
            copy = pltpu.make_async_remote_copy(
                src_ref=sent_rows.at[side],
                dst_ref=got_rows.at[side],
                send_sem=ex_send.at[side],
                recv_sem=ex_recv.at[side],
                device_id={"frag": target},
                device_id_type=MESH,
            )
            copy.start()
            exports.append(copy)
        pending.extend(exports)

    push_amp(0, 1)
    first_half(0, 0, 1)
    first_half(0, 1, 1)
    push_amp(1, 0)
    given = {}
    for turn in range(turns):
        for g in range(groups):
            step = turn * groups + g
            group(step)
            if g == 0:
                if turn > 0:
                    given[turn - 1] = give(turn - 1)
                add_left(turn, step % 2)
            if g == 1 and 0 < turn < turns - 1:
                for r in range((turn - 1) * every, min(turn * every, rounds)):
                    ring_wait(r)
                    if r + 1 < rounds:
                        ring_signal(r + 1)
            if g == groups // 2 - 1 and turn >= 2:
                finish(turn - 2, given[turn - 2])
                if turn - 2 == chunks - 1:
                    make_base(1, step % 2)
                if turn - 2 == (PASSES - 1) * chunks + core_chunks - 1:
                    export()
    given[turns - 1] = give(turns - 1)
    finish(turns - 2, given[turns - 2])
    ends = (frag == 0) | swap
    for i in range(border):
        scale = weight_ref[0, where[core + i]].astype(F32) * 0.5
        product = scale * fold(amp[PASSES, core + i] * exch[core + i])
        energy[0] = energy[0] + jnp.where(ends, product, 0.0)

    def whole(value):
        return jnp.sum(jnp.sum(value, axis=0, keepdims=True), axis=1, keepdims=True)

    lane = lax.broadcasted_iota(jnp.int32, (1, virt), 1)
    sums[device] = jnp.where(lane == 0, whole(energy[0]), 0.0)
    blk_at = [lax.rem(me + j, blocks) for j in range(blocks)]

    def sum_copy(i, j):
        return pltpu.make_async_remote_copy(
            src_ref=sums.at[device],
            dst_ref=sums.at[device],
            send_sem=sum_send.at[i * blocks + j],
            recv_sem=sum_recv.at[i * blocks + j],
            device_id={"frag": lax.rem(frag + i, frags), "blk": blk_at[j]},
            device_id_type=MESH,
        )

    def all_sums(act):
        def some(i, carry):
            for j in range(blocks):
                act(sum_copy(i, j))
            return carry

        lax.fori_loop(1, frags, some, 0)
        for j in range(1, blocks):
            act(sum_copy(0, j))

    all_sums(lambda copy: copy.start())
    finish(turns - 1, given[turns - 1])
    line = jnp.zeros((1, virt), F32)
    for s in range(PASSES):
        line = jnp.where(lane == s, whole(norm_sums[s]), line)
    squares[me] = line
    copies = []
    for j, peer in enumerate(peers):
        copy = pltpu.make_async_remote_copy(
            src_ref=squares.at[me],
            dst_ref=squares.at[me],
            send_sem=sq_send.at[j],
            recv_sem=sq_recv.at[j],
            device_id={"blk": peer},
            device_id_type=MESH,
        )
        copy.start()
        copies.append(copy)
    for copy in exports:
        copy.wait_recv()
    for i in range(border):
        value = amp[PASSES, core + i]
        new_ref[:, i, :] = jnp.where(frag > 0, got_rows[0, i], value)
        new_ref[:, pairs - border + i, :] = jnp.where(swap, value, got_rows[1, i])
    for copy in pending:
        copy.wait_send()
    for copy in copies:
        copy.wait_recv()
    norm_ref[...] = jnp.sqrt(jnp.sum(squares[...], axis=0))[:, :PASSES]
    all_sums(lambda copy: copy.wait_recv())
    total = jnp.sum(sums[...], axis=0)
    energy_ref[...] = -jnp.sum(total, axis=1, keepdims=True) / (virt * virt)
    for copy in copies:
        copy.wait_send()
    all_sums(lambda copy: copy.wait_send())


def on_device(blocks, frags, *args):
    amps, _, factors = args[:3]
    _, rows, pairs, virt = amps.shape
    aux = factors.shape[1]
    border = args[-1].shape[2]
    turns = PASSES * (pairs // CHUNK)
    vmem = pl.BlockSpec(memory_space=pltpu.VMEM)
    hbm = pl.BlockSpec(memory_space=pltpu.HBM)
    dma = pltpu.SemaphoreType.DMA
    new_amps, norms, energy = pl.pallas_call(
        functools.partial(kernel, blocks, frags),
        out_shape=(
            jax.ShapeDtypeStruct(amps.shape[1:], F32),
            jax.ShapeDtypeStruct((1, PASSES), F32),
            jax.ShapeDtypeStruct((1, 1), F32),
        ),
        in_specs=[hbm] * 9,
        out_specs=(vmem, vmem, vmem),
        scratch_shapes=[
            pltpu.VMEM((aux, virt, virt), BF16),
            pltpu.VMEM((rows, pairs, virt), F32),
            pltpu.VMEM((rows, pairs, virt), F32),
            pltpu.VMEM((virt, virt), F32),
            pltpu.VMEM((1, virt), F32),
            pltpu.SMEM((1, pairs, pairs), F32),
            pltpu.SMEM((1, pairs), F32),
            pltpu.SMEM((1, pairs), jnp.int32),
            pltpu.SMEM((1, 2, border), jnp.int32),
            pltpu.VMEM((PASSES + 1, pairs, rows, virt), F32),
            pltpu.VMEM((PASSES, blocks, pairs, rows, virt), BF16),
            pltpu.VMEM((UNITS, 2, CHUNK, 2, virt, virt), BF16),
            pltpu.VMEM((turns, blocks, CHUNK, rows, virt), F32),
            pltpu.VMEM((turns, blocks - 1, CHUNK, rows, virt), F32),
            pltpu.VMEM((blocks, CHUNK, rows, virt), BF16),
            pltpu.VMEM((blocks - 1, CHUNK, rows, virt), BF16),
            pltpu.VMEM((pairs, rows, virt), F32),
            pltpu.VMEM((PASSES, pairs, rows, virt), F32),
            pltpu.VMEM((pairs, rows, virt), F32),
            pltpu.VMEM((virt, 2 * virt), BF16),
            pltpu.VMEM((virt, 2 * virt), BF16),
            pltpu.VMEM((rows, virt), F32),
            pltpu.VMEM((virt, virt), F32),
            pltpu.VMEM((2, border, rows, virt), F32),
            pltpu.VMEM((2, border, rows, virt), F32),
            pltpu.VMEM((2, border, rows, virt), F32),
            pltpu.VMEM((2, border, rows, virt), F32),
            pltpu.VMEM((blocks * frags, 1, virt), F32),
            pltpu.VMEM((blocks, 1, virt), F32),
            pltpu.SemaphoreType.REGULAR((frags // 2, 2)),
            dma((8,)),
            dma((aux // GROUP,)),
            dma((turns, blocks - 1)),
            dma((turns, blocks - 1)),
            dma((turns, blocks - 1)),
            dma((turns, blocks - 1)),
            dma((2,)),
            dma((2,)),
            dma((2,)),
            dma((2,)),
            dma((blocks * frags,)),
            dma((blocks * frags,)),
            dma((blocks - 1,)),
            dma((blocks - 1,)),
        ],
        compiler_params=pltpu.CompilerParams(
            collective_id=0, has_side_effects=True, vmem_limit_bytes=48 * 2**20
        ),
    )(*[pltpu.with_memory_space_constraint(x, pltpu.HBM) for x in args])
    return new_amps.reshape(amps.shape), norms, energy.reshape(())


def solution(mesh):
    placed = (
        P("frag", "blk", None, None),
        P("frag", "blk", None, None),
        P("frag", "blk", None, None),
        P("frag", None, None),
        P("frag", None, None),
        P("frag", None),
        P("frag", None),
        P("frag", None),
        P("frag", None, None),
    )
    return jax.shard_map(
        functools.partial(on_device, mesh.shape["blk"], mesh.shape["frag"]),
        mesh=mesh,
        in_specs=placed,
        out_specs=(P("frag", "blk", None, None), P("frag", None), P()),
        check_vma=False,
    )
```

```python
import functools

import jax
import jax.numpy as jnp
from jax import lax
from jax.experimental import pallas as pl
from jax.experimental.pallas import tpu as pltpu
from jax.sharding import PartitionSpec as P

PASSES = 2
CHUNK = 2
UNITS = 2
GROUP = 8
GIVE = 1
FINISH = 6
MESH = pl.DeviceIdType.MESH
F32, BF16 = jnp.float32, jnp.bfloat16


def halves(value):
    high = value.astype(BF16)
    return high, (value - high.astype(F32)).astype(BF16)


def kernel(blocks, frags, *refs):
    virt = refs[0].shape[3]
    tall, flat = (2 * virt, 2 * virt), (virt, 2 * virt)

    def body(first, ladder, left, right):
        run(blocks, frags, first, ladder, left, right, *refs)

    pl.run_scoped(
        body,
        [[pltpu.ACC(m)(tall, F32) for _ in range(2)] for m in range(UNITS)],
        [[pltpu.ACC(m)(flat, F32) for _ in range(2)] for m in range(UNITS)],
        [pltpu.ACC(m)(flat, F32) for m in range(UNITS)],
        [pltpu.ACC(m)(flat, F32) for m in range(UNITS)],
    )


def run(
    blocks,
    frags,
    first_acc,
    ladder_acc,
    left_acc,
    right_acc,
    amps_hbm,
    exch_hbm,
    factors_hbm,
    hole_hbm,
    fock_hbm,
    orbital_hbm,
    pair_hbm,
    weight_hbm,
    export_hbm,
    new_ref,
    line_ref,
    fact,
    amps_in,
    exch_in,
    fock_in,
    orbital_in,
    hole_ref,
    pair_ref,
    weight_ref,
    export_ref,
    amp,
    low,
    half,
    part,
    recv,
    part_low,
    recv_low,
    exch,
    base,
    recip,
    fock_row,
    fock_col,
    row_energy,
    row_t,
    sent_rows,
    got_rows,
    sent_weights,
    got_weights,
    sums,
    squares,
    ring,
    in_sem,
    fact_sem,
    ag_send,
    ag_recv,
    rs_send,
    rs_recv,
    ex_send,
    ex_recv,
    we_send,
    we_recv,
    sum_send,
    sum_recv,
    sq_send,
    sq_recv,
):
    me = lax.axis_index("blk")
    frag = lax.axis_index("frag")
    rows, pairs, virt = amps_in.shape
    aux = fact.shape[0]
    groups = aux // GROUP
    border = export_hbm.shape[2]
    device = frag * blocks + me
    peers = [lax.rem(me + j, blocks) for j in range(1, blocks)]
    core = pairs - 2 * border
    swap = frag == frags - 1

    def pair_at(place):
        if place < core:
            return border + place
        at = (place - core) % border
        lower, upper = at, pairs - border + at
        if place - core < border:
            return jnp.where(swap, upper, lower)
        return jnp.where(swap, lower, upper)

    def take(ref, place):
        if place < core:
            return ref[:, border + place, :]
        at = (place - core) % border
        lower, upper = ref[:, at, :], ref[:, pairs - border + at, :]
        if place - core < border:
            return jnp.where(swap, upper, lower)
        return jnp.where(swap, lower, upper)

    chunks = pairs // CHUNK
    core_chunks = core // CHUNK
    turns = PASSES * chunks
    count = turns * groups

    def place(turn):
        return turn // chunks, turn % chunks * CHUNK

    sides = [lax.rem(frag + frags - 1, frags), lax.rem(frag + 1, frags)]

    def joint(ref, send_sem, recv_sem):
        return pltpu.make_async_remote_copy(
            src_ref=ref,
            dst_ref=ref,
            send_sem=send_sem,
            recv_sem=recv_sem,
            device_id={"blk": peers[0]},
            device_id_type=MESH,
        )

    loads = []
    for i, (src, dst) in enumerate(
        (
            (amps_hbm.at[0], amps_in),
            (fock_hbm.at[0], fock_in),
            (orbital_hbm, orbital_in),
            (pair_hbm, pair_ref),
            (hole_hbm, hole_ref),
            (exch_hbm.at[0], exch_in),
            (weight_hbm, weight_ref),
            (export_hbm, export_ref),
        )
    ):
        loads.append(pltpu.make_async_copy(src, dst, in_sem.at[i]))
    fact_load = pltpu.make_async_copy(factors_hbm.at[0], fact, fact_sem)
    for copy in loads:
        copy.start()
    fact_load.start()

    barrier = pltpu.get_barrier_semaphore()

    for peer in peers:
        pl.semaphore_signal(barrier, inc=1, device_id={"blk": peer}, device_id_type=MESH)
    for side in sides:
        pl.semaphore_signal(barrier, inc=1, device_id={"frag": side}, device_id_type=MESH)

    rounds = frags // 2
    every = pl.cdiv(rounds, turns - 3)

    def ring_signal():
        for i, side in enumerate(sides):
            pl.semaphore_signal(
                ring.at[i], inc=1, device_id={"frag": side}, device_id_type=MESH
            )

    def ring_wait():
        for i in range(2):
            pl.semaphore_wait(ring.at[i], 1)

    for m in range(UNITS):
        for ref in first_acc[m] + ladder_acc[m] + [left_acc[m], right_acc[m]]:
            pltpu.matmul_pop(ref)

    loads[0].wait()

    def enter(place):
        value = take(amps_in, place)
        amp[0, place] = value
        low[0, me, place] = value.astype(BF16)

    for place_at in range(CHUNK):
        enter(place_at)
    pl.semaphore_wait(barrier, blocks - 1 + 2)

    pending = []

    def gather(turn):
        sweep, start = place(turn)
        where = low.at[sweep, me, pl.ds(start, CHUNK)]
        for peer in peers:
            pltpu.make_async_remote_copy(
                src_ref=where,
                dst_ref=where,
                send_sem=ag_send.at[turn],
                recv_sem=ag_recv.at[turn],
                device_id={"blk": peer},
                device_id_type=MESH,
            ).start()
        span = low.at[sweep, pl.ds(0, blocks - 1), pl.ds(start, CHUNK)]
        pending.append(joint(span, ag_send.at[turn], ag_recv.at[turn]))
        return pending[-1]

    gathers = {0: gather(0)}
    for turn in range(1, chunks):
        for i in range(CHUNK):
            enter(turn * CHUNK + i)
        gathers[turn] = gather(turn)

    def scatter(turn):
        last = turn == turns - 1
        source, target = (part_low, recv_low) if last else (part.at[turn], recv.at[turn])
        for j, peer in enumerate(peers):
            pltpu.make_async_remote_copy(
                src_ref=source.at[peer],
                dst_ref=target.at[j],
                send_sem=rs_send.at[turn],
                recv_sem=rs_recv.at[turn],
                device_id={"blk": peer},
                device_id_type=MESH,
            ).start()
        pending.append(joint(target, rs_send.at[turn], rs_recv.at[turn]))
        return pending[-1]

    offset = pl.multiple_of(me * rows, rows)
    for copy in loads[1:5]:
        copy.wait()
    column = lax.broadcasted_iota(jnp.int32, (virt, virt), 1)
    own = (column >= offset) & (column < offset + rows)
    high, middle = halves(fock_in[...])
    fock_row[:, :virt] = high
    fock_row[:, virt:] = middle
    high, middle = halves(jnp.where(own, fock_in[...], 0.0))
    fock_col[:, :virt] = high
    fock_col[:, virt:] = middle
    row_t[...] = jnp.broadcast_to(orbital_in[...], (virt, virt)).T
    row_energy[...] = row_t[pl.ds(offset, rows), :] + orbital_in[...]
    where = [pair_at(p) for p in range(pairs)]
    levels = [pair_ref[0, p] for p in where]
    for p in range(pairs):
        recip[p] = 1.0 / (row_energy[...] - levels[p])
    for copy in loads[5:]:
        copy.wait()
    weights = [weight_ref[0, p].astype(F32) * 0.5 for p in range(pairs)]
    for p in range(pairs):
        exch[p] = take(exch_in, p)
    for i, side in enumerate(sides):
        for r in range(border):
            p = r if i == 0 else pairs - border + r
            sent_weights[i, r] = exch_in[:, p, :] * weights[p]
    for i, side in enumerate(sides):
        pltpu.make_async_remote_copy(
            src_ref=sent_weights.at[i],
            dst_ref=got_weights.at[i],
            send_sem=we_send,
            recv_sem=we_recv,
            device_id={"frag": side},
            device_id_type=MESH,
        ).start()
    weight_copy = joint(got_weights, we_send, we_recv)
    pending.append(weight_copy)
    ring_signal()

    def make_base(sweep, register):
        share = pairs // UNITS
        tile = jnp.concatenate([fock_row[...], jnp.zeros((virt, 2 * virt), BF16)], axis=0)
        for m in range(UNITS):
            pltpu.matmul_push_rhs(tile, staging_register=register, mxu_index=m, transpose=True)
        for m in range(UNITS):
            split = halves(amp[sweep, m * share : (m + 1) * share].reshape(share * rows, virt))
            for i, value in enumerate(split):
                pltpu.matmul_acc_lhs(
                    right_acc[m],
                    jnp.concatenate([value, value], axis=1),
                    load_staged_rhs=register if i == 0 else None,
                )
        for m in range(UNITS):
            product = pltpu.matmul_pop(right_acc[m])
            for k in range(share):
                p = m * share + k
                total = exch[p] + product[k * rows : (k + 1) * rows, :virt]
                for r in range(pairs):
                    total = total + hole_ref[0, where[p], where[r]] * amp[sweep, r]
                total = total - (row_energy[...] - levels[p]) * amp[sweep, p]
                base[sweep, p] = total

    make_base(0, 0)

    def add_left(turn, register):
        sweep, start = place(turn)
        split = [halves(amp[sweep, start + i]) for i in range(CHUNK)]
        for m in range(UNITS):
            tile = jnp.concatenate([split[i][m] for i in range(CHUNK)], axis=1)
            tile = jnp.concatenate([tile] * (2 * blocks), axis=0)
            pltpu.matmul_push_rhs(tile, staging_register=register, mxu_index=m)
            pltpu.matmul_acc_lhs(left_acc[m], fock_col[...], load_staged_rhs=register)

    def aux_at(step, m, i):
        return (step % groups) * GROUP + m * (GROUP // UNITS) + 2 * i

    def push_amp(step, register):
        turn = step // groups
        sweep, start = place(turn)
        if step % groups == 0:
            gathers[turn].wait_recv()
        tile = jnp.concatenate(
            [low[sweep, :, start + i].reshape(virt, virt) for i in range(CHUNK)], axis=1
        )
        tile = jnp.concatenate([tile, jnp.zeros((virt, 2 * virt), BF16)], axis=0)
        for m in range(UNITS):
            pltpu.matmul_push_rhs(tile, staging_register=register, mxu_index=m)

    def first_half(step, i, register):
        if step == 0 and i == 0:
            fact_load.wait()
        for m in range(UNITS):
            q = aux_at(step, m, i)
            slab = fact[q : q + 2].reshape(2 * virt, virt)
            pltpu.matmul_acc_lhs(
                first_acc[m][i],
                jnp.concatenate([slab, jnp.zeros_like(slab)], axis=1),
                load_staged_rhs=register if i == 0 else None,
            )

    def turn_half(i, register):
        for m in range(UNITS):
            done = pltpu.matmul_pop(first_acc[m][i]).astype(BF16)
            for p in range(CHUNK):
                for q in range(2):
                    half[m, i, p, q] = done[q * virt : (q + 1) * virt, p * virt : (p + 1) * virt]

    def push_half(i, register):
        for m in range(UNITS):
            tile = jnp.concatenate(
                [
                    jnp.concatenate([half[m, i, p, q] for q in range(2)], axis=1)
                    for p in range(CHUNK)
                ],
                axis=0,
            )
            pltpu.matmul_push_rhs(tile, staging_register=register, mxu_index=m, transpose=True)

    def second_half(step, i, register):
        turn = step // groups
        for m in range(UNITS):
            q = aux_at(step, m, i)
            pltpu.matmul_acc_lhs(
                ladder_acc[m][turn % 2],
                jnp.concatenate([fact[q], fact[q + 1]], axis=1),
                load_staged_rhs=register,
            )

    def group(step):
        now, free = step % 2, 1 - step % 2
        more = step + 1 < count
        turn_half(0, free)
        if more:
            first_half(step + 1, 0, now)
        push_half(0, free)
        turn_half(1, now)
        if more:
            first_half(step + 1, 1, now)
        push_half(1, now)
        second_half(step, 0, free)
        if step + 2 < count:
            push_amp(step + 2, free)
        second_half(step, 1, now)

    def give(turn):
        total = pltpu.matmul_pop(ladder_acc[0][turn % 2])
        side = pltpu.matmul_pop(left_acc[0])
        for m in range(1, UNITS):
            total = total + pltpu.matmul_pop(ladder_acc[m][turn % 2])
            side = side + pltpu.matmul_pop(left_acc[m])
        for i in range(CHUNK):
            cols = slice(i * virt, (i + 1) * virt)
            value = total[:, cols].T + side[:, cols]
            for k in range(blocks):
                piece = value[k * rows : (k + 1) * rows]
                part[turn, k, i] = piece
                if turn == turns - 1:
                    part_low[k, i] = piece.astype(BF16)
        return scatter(turn)

    norm_sums = [jnp.zeros((8, virt), F32) for _ in range(PASSES)]
    energy = [jnp.zeros((8, virt), F32)]

    def fold(value):
        return jnp.sum(value.reshape(rows // 8, 8, virt), axis=0)

    def finish(turn):
        sweep, start = place(turn)
        last = turn == turns - 1
        for i in range(CHUNK):
            p = start + i
            residual = base[sweep, p] + part[turn, me, i]
            for j in range(blocks - 1):
                residual = residual + (recv_low[j, i].astype(F32) if last else recv[turn, j, i])
            norm_sums[sweep] += fold(residual * residual)
            if last:
                continue
            value = amp[sweep, p] + residual * recip[p]
            amp[sweep + 1, p] = value
            if sweep + 1 < PASSES:
                low[sweep + 1, me, p] = value.astype(BF16)
            elif p < core:
                new_ref[:, border + p, :] = value
                energy[0] = energy[0] + weights[border + p] * fold(value * exch[p])
        if sweep + 1 < PASSES:
            gathers[turn + chunks] = gather(turn + chunks)

    exports = []

    def export():
        weight_copy.wait_recv()
        for side, target in ((0, sides[1]), (1, sides[0])):
            used = frag < frags - 1 if side == 0 else frag > 0
            for r in range(border):
                value = amp[PASSES, jnp.maximum(export_ref[0, side, r] - border, 0)]
                sent_rows[side, r] = value
                energy[0] = energy[0] + jnp.where(used, fold(value * got_weights[side, r]), 0.0)
            pltpu.make_async_remote_copy(
                src_ref=sent_rows.at[side],
                dst_ref=got_rows.at[side],
                send_sem=ex_send,
                recv_sem=ex_recv,
                device_id={"frag": target},
                device_id_type=MESH,
            ).start()
        exports.append(joint(got_rows, ex_send, ex_recv))
        pending.extend(exports)

    push_amp(0, 1)
    first_half(0, 0, 1)
    first_half(0, 1, 1)
    push_amp(1, 0)
    given = {}
    ring_turn = turns - 1 - pl.cdiv(rounds, every)
    for turn in range(turns):
        for g in range(groups):
            step = turn * groups + g
            if g == FINISH and turn >= 2:
                given[turn - 2].wait_recv()
            group(step)
            if g == GIVE:
                if turn > 0:
                    given[turn - 1] = give(turn - 1)
                if ring_turn <= turn < turns - 1:
                    at = (turn - ring_turn) * every
                    for r in range(at, min(at + every, rounds)):
                        ring_wait()
                        if r + 1 < rounds:
                            ring_signal()
                add_left(turn, step % 2)
            if g == FINISH and turn >= 2:
                finish(turn - 2)
                if turn - 2 == chunks - 1:
                    make_base(1, step % 2)
                if turn - 2 == (PASSES - 1) * chunks + core_chunks - 1:
                    export()
    given[turns - 1] = give(turns - 1)
    given[turns - 2].wait_recv()
    finish(turns - 2)
    ends = (frag == 0) | swap
    for i in range(border):
        scale = weight_ref[0, where[core + i]].astype(F32) * 0.5
        product = scale * fold(amp[PASSES, core + i] * exch[core + i])
        energy[0] = energy[0] + jnp.where(ends, product, 0.0)

    def whole(value):
        return jnp.sum(jnp.sum(value, axis=0, keepdims=True), axis=1, keepdims=True)

    lane = lax.broadcasted_iota(jnp.int32, (1, virt), 1)
    sums[device] = jnp.where(lane == 0, whole(energy[0]), 0.0)
    blk_at = [lax.rem(me + j, blocks) for j in range(blocks)]

    def send_sum(i, j):
        pltpu.make_async_remote_copy(
            src_ref=sums.at[device],
            dst_ref=sums.at[device],
            send_sem=sum_send,
            recv_sem=sum_recv,
            device_id={"frag": lax.rem(frag + i, frags), "blk": blk_at[j]},
            device_id_type=MESH,
        ).start()

    def send_sums(i, carry):
        for j in range(blocks):
            send_sum(i, j)
        return carry

    lax.fori_loop(1, frags, send_sums, 0)
    for j in range(1, blocks):
        send_sum(0, j)
    sum_copy = joint(sums.at[pl.ds(0, blocks * frags - 1)], sum_send, sum_recv)
    given[turns - 1].wait_recv()
    finish(turns - 1)
    line = jnp.zeros((1, virt), F32)
    for s in range(PASSES):
        line = jnp.where(lane == s, whole(norm_sums[s]), line)
    squares[me] = line
    for peer in peers:
        pltpu.make_async_remote_copy(
            src_ref=squares.at[me],
            dst_ref=squares.at[me],
            send_sem=sq_send,
            recv_sem=sq_recv,
            device_id={"blk": peer},
            device_id_type=MESH,
        ).start()
    square_copy = joint(squares.at[pl.ds(0, blocks - 1)], sq_send, sq_recv)
    for copy in exports:
        copy.wait_recv()
    for i in range(border):
        value = amp[PASSES, core + i]
        new_ref[:, i, :] = jnp.where(frag > 0, got_rows[0, i], value)
        new_ref[:, pairs - border + i, :] = jnp.where(swap, value, got_rows[1, i])
    for copy in pending:
        copy.wait_send()
    sum_copy.wait_send()
    square_copy.wait_recv()
    roots = jnp.sqrt(jnp.sum(squares[...], axis=0))
    sum_copy.wait_recv()
    total = jnp.sum(sums[...], axis=0)
    scaled = -jnp.sum(total, axis=1, keepdims=True) / (virt * virt)
    line_ref[...] = jnp.where(lane == PASSES, scaled, roots)
    square_copy.wait_send()


def hand_out(new_ref, line_ref, new_out, norm_out, energy_out, norm, energy, sem):
    first = pltpu.make_async_copy(new_ref, new_out, sem.at[0])
    first.start()
    norm[...] = line_ref[:, :PASSES]
    energy[...] = line_ref[:, PASSES : PASSES + 1]
    copies = [
        pltpu.make_async_copy(norm, norm_out, sem.at[1]),
        pltpu.make_async_copy(energy, energy_out, sem.at[2]),
    ]
    for copy in copies:
        copy.start()
    for copy in [first] + copies:
        copy.wait()


def on_device(blocks, frags, *args):
    amps, _, factors = args[:3]
    _, rows, pairs, virt = amps.shape
    aux = factors.shape[1]
    border = args[-1].shape[2]
    turns = PASSES * (pairs // CHUNK)
    vmem = pl.BlockSpec(memory_space=pltpu.VMEM)
    hbm = pl.BlockSpec(memory_space=pltpu.HBM)
    dma = pltpu.SemaphoreType.DMA
    new_amps, line = pl.pallas_call(
        functools.partial(kernel, blocks, frags),
        out_shape=(
            jax.ShapeDtypeStruct(amps.shape[1:], F32),
            jax.ShapeDtypeStruct((1, virt), F32),
        ),
        in_specs=[hbm] * 9,
        out_specs=(vmem, vmem),
        scratch_shapes=[
            pltpu.VMEM((aux, virt, virt), BF16),
            pltpu.VMEM((rows, pairs, virt), F32),
            pltpu.VMEM((rows, pairs, virt), F32),
            pltpu.VMEM((virt, virt), F32),
            pltpu.VMEM((1, virt), F32),
            pltpu.SMEM((1, pairs, pairs), F32),
            pltpu.SMEM((1, pairs), F32),
            pltpu.SMEM((1, pairs), jnp.int32),
            pltpu.SMEM((1, 2, border), jnp.int32),
            pltpu.VMEM((PASSES + 1, pairs, rows, virt), F32),
            pltpu.VMEM((PASSES, blocks, pairs, rows, virt), BF16),
            pltpu.VMEM((UNITS, 2, CHUNK, 2, virt, virt), BF16),
            pltpu.VMEM((turns, blocks, CHUNK, rows, virt), F32),
            pltpu.VMEM((turns, blocks - 1, CHUNK, rows, virt), F32),
            pltpu.VMEM((blocks, CHUNK, rows, virt), BF16),
            pltpu.VMEM((blocks - 1, CHUNK, rows, virt), BF16),
            pltpu.VMEM((pairs, rows, virt), F32),
            pltpu.VMEM((PASSES, pairs, rows, virt), F32),
            pltpu.VMEM((pairs, rows, virt), F32),
            pltpu.VMEM((virt, 2 * virt), BF16),
            pltpu.VMEM((virt, 2 * virt), BF16),
            pltpu.VMEM((rows, virt), F32),
            pltpu.VMEM((virt, virt), F32),
            pltpu.VMEM((2, border, rows, virt), F32),
            pltpu.VMEM((2, border, rows, virt), F32),
            pltpu.VMEM((2, border, rows, virt), F32),
            pltpu.VMEM((2, border, rows, virt), F32),
            pltpu.VMEM((blocks * frags, 1, virt), F32),
            pltpu.VMEM((blocks, 1, virt), F32),
            pltpu.SemaphoreType.REGULAR((2,)),
            dma((8,)),
            dma,
            dma((turns,)),
            dma((turns,)),
            dma((turns,)),
            dma((turns,)),
            dma,
            dma,
            dma,
            dma,
            dma,
            dma,
            dma,
            dma,
        ],
        compiler_params=pltpu.CompilerParams(
            collective_id=0, has_side_effects=True, vmem_limit_bytes=48 * 2**20
        ),
    )(*[pltpu.with_memory_space_constraint(x, pltpu.HBM) for x in args])
    shapes = (new_amps.shape, (1, PASSES), (1, 1))
    new_amps, norms, energy = pl.pallas_call(
        hand_out,
        out_shape=tuple(jax.ShapeDtypeStruct(shape, F32) for shape in shapes),
        in_specs=[vmem] * 2,
        out_specs=(pl.BlockSpec(memory_space=pl.ANY),) * 3,
        scratch_shapes=[pltpu.VMEM(shape, F32) for shape in shapes[1:]] + [dma((3,))],
        compiler_params=pltpu.CompilerParams(vmem_limit_bytes=2**20),
    )(new_amps, line)
    return new_amps.reshape(amps.shape), norms, energy.reshape(())


def solution(mesh):
    placed = (
        P("frag", "blk", None, None),
        P("frag", "blk", None, None),
        P("frag", "blk", None, None),
        P("frag", None, None),
        P("frag", None, None),
        P("frag", None),
        P("frag", None),
        P("frag", None),
        P("frag", None, None),
    )
    return jax.shard_map(
        functools.partial(on_device, mesh.shape["blk"], mesh.shape["frag"]),
        mesh=mesh,
        in_specs=placed,
        out_specs=(P("frag", "blk", None, None), P("frag", None), P()),
        check_vma=False,
    )
```

```python
import functools

import jax
import jax.numpy as jnp
from jax import lax
from jax.experimental import pallas as pl
from jax.experimental.pallas import tpu as pltpu
from jax.sharding import PartitionSpec as P

PASSES = 2
CHUNK = 2
UNITS = 2
GROUP = 8
GIVE = 1
LAST_GIVE = 0
FINISH = 6
MESH = pl.DeviceIdType.MESH
F32, BF16 = jnp.float32, jnp.bfloat16


def halves(value):
    high = value.astype(BF16)
    return high, (value - high.astype(F32)).astype(BF16)


def kernel(blocks, frags, *refs):
    virt = refs[0].shape[3]
    tall, flat = (2 * virt, 2 * virt), (virt, 2 * virt)

    turns = PASSES * (refs[0].shape[2] // CHUNK)
    dma = pltpu.SemaphoreType.DMA

    def body(first, ladder, left, right, semaphores):
        run(blocks, frags, first, ladder, left, right, *refs, *semaphores)

    pl.run_scoped(
        body,
        [[pltpu.ACC(m)(tall, F32) for _ in range(2)] for m in range(UNITS)],
        [[pltpu.ACC(m)(flat, F32) for _ in range(2)] for m in range(UNITS)],
        [pltpu.ACC(m)(flat, F32) for m in range(UNITS)],
        [pltpu.ACC(m)(flat, F32) for m in range(UNITS)],
        [pltpu.SemaphoreType.REGULAR((2,)), dma((8,)), dma] + [dma((turns,))] * 4 + [dma] * 8,
    )


def run(
    blocks,
    frags,
    first_acc,
    ladder_acc,
    left_acc,
    right_acc,
    amps_hbm,
    exch_hbm,
    factors_hbm,
    hole_hbm,
    fock_hbm,
    orbital_hbm,
    pair_hbm,
    weight_hbm,
    export_hbm,
    new_ref,
    line_ref,
    fact,
    amps_in,
    exch_in,
    fock_in,
    orbital_in,
    hole_ref,
    pair_ref,
    weight_ref,
    export_ref,
    amp,
    low,
    half,
    part,
    recv,
    part_low,
    recv_low,
    exch,
    base,
    recip,
    fock_row,
    fock_col,
    row_energy,
    row_t,
    sent_rows,
    got_rows,
    sent_weights,
    got_weights,
    sums,
    squares,
    ring,
    in_sem,
    fact_sem,
    ag_send,
    ag_recv,
    rs_send,
    rs_recv,
    ex_send,
    ex_recv,
    we_send,
    we_recv,
    sum_send,
    sum_recv,
    sq_send,
    sq_recv,
):
    me = lax.axis_index("blk")
    frag = lax.axis_index("frag")
    rows, pairs, virt = amps_in.shape
    aux = fact.shape[0]
    groups = aux // GROUP
    border = export_hbm.shape[2]
    device = frag * blocks + me
    peers = [lax.rem(me + j, blocks) for j in range(1, blocks)]
    core = pairs - 2 * border
    swap = frag == frags - 1

    def pair_at(place):
        if place < core:
            return border + place
        at = (place - core) % border
        lower, upper = at, pairs - border + at
        if place - core < border:
            return jnp.where(swap, upper, lower)
        return jnp.where(swap, lower, upper)

    def take(ref, place):
        if place < core:
            return ref[:, border + place, :]
        at = (place - core) % border
        lower, upper = ref[:, at, :], ref[:, pairs - border + at, :]
        if place - core < border:
            return jnp.where(swap, upper, lower)
        return jnp.where(swap, lower, upper)

    chunks = pairs // CHUNK
    core_chunks = core // CHUNK
    turns = PASSES * chunks
    count = turns * groups

    def place(turn):
        return turn // chunks, turn % chunks * CHUNK

    sides = [lax.rem(frag + frags - 1, frags), lax.rem(frag + 1, frags)]

    def joint(ref, send_sem, recv_sem):
        return pltpu.make_async_remote_copy(
            src_ref=ref,
            dst_ref=ref,
            send_sem=send_sem,
            recv_sem=recv_sem,
            device_id={"blk": peers[0]},
            device_id_type=MESH,
        )

    loads = []
    for i, (src, dst) in enumerate(
        (
            (amps_hbm.at[0], amps_in),
            (fock_hbm.at[0], fock_in),
            (orbital_hbm, orbital_in),
            (pair_hbm, pair_ref),
            (hole_hbm, hole_ref),
            (exch_hbm.at[0], exch_in),
            (weight_hbm, weight_ref),
            (export_hbm, export_ref),
        )
    ):
        loads.append(pltpu.make_async_copy(src, dst, in_sem.at[i]))
    fact_load = pltpu.make_async_copy(factors_hbm.at[0], fact, fact_sem)
    for copy in loads:
        copy.start()
    fact_load.start()

    barrier = pltpu.get_barrier_semaphore()

    for peer in peers:
        pl.semaphore_signal(barrier, inc=1, device_id={"blk": peer}, device_id_type=MESH)
    for side in sides:
        pl.semaphore_signal(barrier, inc=1, device_id={"frag": side}, device_id_type=MESH)

    rounds = frags // 2
    every = pl.cdiv(rounds, turns - 3)

    def ring_signal():
        for i, side in enumerate(sides):
            pl.semaphore_signal(
                ring.at[i], inc=1, device_id={"frag": side}, device_id_type=MESH
            )

    def ring_wait():
        for i in range(2):
            pl.semaphore_wait(ring.at[i], 1)

    for m in range(UNITS):
        for ref in first_acc[m] + ladder_acc[m] + [left_acc[m], right_acc[m]]:
            pltpu.matmul_pop(ref)

    loads[0].wait()

    def enter(place):
        value = take(amps_in, place)
        amp[0, place] = value
        low[0, me, place] = value.astype(BF16)

    for place_at in range(CHUNK):
        enter(place_at)
    pl.semaphore_wait(barrier, blocks - 1 + 2)

    pending = []

    def gather(turn):
        sweep, start = place(turn)
        where = low.at[sweep, me, pl.ds(start, CHUNK)]
        for peer in peers:
            pltpu.make_async_remote_copy(
                src_ref=where,
                dst_ref=where,
                send_sem=ag_send.at[turn],
                recv_sem=ag_recv.at[turn],
                device_id={"blk": peer},
                device_id_type=MESH,
            ).start()
        span = low.at[sweep, pl.ds(0, blocks - 1), pl.ds(start, CHUNK)]
        pending.append(joint(span, ag_send.at[turn], ag_recv.at[turn]))
        return pending[-1]

    gathers = {0: gather(0)}
    for turn in range(1, chunks):
        for i in range(CHUNK):
            enter(turn * CHUNK + i)
        gathers[turn] = gather(turn)

    def scatter(turn):
        last = turn == turns - 1
        source, target = (part_low, recv_low) if last else (part.at[turn], recv.at[turn])
        for j, peer in enumerate(peers):
            pltpu.make_async_remote_copy(
                src_ref=source.at[peer],
                dst_ref=target.at[j],
                send_sem=rs_send.at[turn],
                recv_sem=rs_recv.at[turn],
                device_id={"blk": peer},
                device_id_type=MESH,
            ).start()
        pending.append(joint(target, rs_send.at[turn], rs_recv.at[turn]))
        return pending[-1]

    offset = pl.multiple_of(me * rows, rows)
    for copy in loads[1:5]:
        copy.wait()
    column = lax.broadcasted_iota(jnp.int32, (virt, virt), 1)
    own = (column >= offset) & (column < offset + rows)
    high, middle = halves(fock_in[...])
    fock_row[:, :virt] = high
    fock_row[:, virt:] = middle
    high, middle = halves(jnp.where(own, fock_in[...], 0.0))
    fock_col[:, :virt] = high
    fock_col[:, virt:] = middle
    row_t[...] = jnp.broadcast_to(orbital_in[...], (virt, virt)).T
    row_energy[...] = row_t[pl.ds(offset, rows), :] + orbital_in[...]
    where = [pair_at(p) for p in range(pairs)]
    levels = [pair_ref[0, p] for p in where]
    for p in range(pairs):
        recip[p] = 1.0 / (row_energy[...] - levels[p])
    for copy in loads[5:]:
        copy.wait()
    weights = [weight_ref[0, p].astype(F32) * 0.5 for p in range(pairs)]
    for p in range(pairs):
        exch[p] = take(exch_in, p)
    for i, side in enumerate(sides):
        for r in range(border):
            p = r if i == 0 else pairs - border + r
            sent_weights[i, r] = exch_in[:, p, :] * weights[p]
    for i, side in enumerate(sides):
        pltpu.make_async_remote_copy(
            src_ref=sent_weights.at[i],
            dst_ref=got_weights.at[i],
            send_sem=we_send,
            recv_sem=we_recv,
            device_id={"frag": side},
            device_id_type=MESH,
        ).start()
    weight_copy = joint(got_weights, we_send, we_recv)
    pending.append(weight_copy)
    ring_signal()

    def add_hole(sweep, places, fresh):
        for p in range(pairs):
            total = exch[p] if fresh else base[sweep, p]
            for r in places:
                total = total + hole_ref[0, where[p], where[r]] * amp[sweep, r]
                if r == p:
                    total = total - (row_energy[...] - levels[p]) * amp[sweep, p]
            base[sweep, p] = total

    share = pairs // UNITS

    def push_fock(register):
        tile = jnp.concatenate([fock_row[...], jnp.zeros((virt, 2 * virt), BF16)], axis=0)
        for m in range(UNITS):
            pltpu.matmul_push_rhs(tile, staging_register=register, mxu_index=m, transpose=True)

    def add_right(sweep, register):
        for m in range(UNITS):
            split = halves(amp[sweep, m * share : (m + 1) * share].reshape(share * rows, virt))
            for i, value in enumerate(split):
                pltpu.matmul_acc_lhs(
                    right_acc[m],
                    jnp.concatenate([value, value], axis=1),
                    load_staged_rhs=register if i == 0 else None,
                )

    def take_right(sweep):
        for m in range(UNITS):
            product = pltpu.matmul_pop(right_acc[m])
            for k in range(share):
                p = m * share + k
                base[sweep, p] += product[k * rows : (k + 1) * rows, :virt]

    push_fock(0)
    add_right(0, 0)
    add_hole(0, range(pairs), True)
    take_right(0)

    def push_left(turn, register):
        sweep, start = place(turn)
        split = [halves(amp[sweep, start + i]) for i in range(CHUNK)]
        for m in range(UNITS):
            tile = jnp.concatenate([split[i][m] for i in range(CHUNK)], axis=1)
            tile = jnp.concatenate([tile] * (2 * blocks), axis=0)
            pltpu.matmul_push_rhs(tile, staging_register=register, mxu_index=m)

    def add_left(register):
        for m in range(UNITS):
            pltpu.matmul_acc_lhs(left_acc[m], fock_col[...], load_staged_rhs=register)

    def aux_at(step, m, i):
        return (step % groups) * GROUP + m * (GROUP // UNITS) + 2 * i

    def push_amp(step, register):
        turn = step // groups
        sweep, start = place(turn)
        if step % groups == 0:
            gathers[turn].wait_recv()
        tile = jnp.concatenate(
            [low[sweep, :, start + i].reshape(virt, virt) for i in range(CHUNK)], axis=1
        )
        tile = jnp.concatenate([tile, jnp.zeros((virt, 2 * virt), BF16)], axis=0)
        for m in range(UNITS):
            pltpu.matmul_push_rhs(tile, staging_register=register, mxu_index=m)

    def first_half(step, i, register):
        if step == 0 and i == 0:
            fact_load.wait()
        for m in range(UNITS):
            q = aux_at(step, m, i)
            slab = fact[q : q + 2].reshape(2 * virt, virt)
            pltpu.matmul_acc_lhs(
                first_acc[m][i],
                jnp.concatenate([slab, jnp.zeros_like(slab)], axis=1),
                load_staged_rhs=register if i == 0 else None,
            )

    def turn_half(i, register):
        for m in range(UNITS):
            done = pltpu.matmul_pop(first_acc[m][i]).astype(BF16)
            for p in range(CHUNK):
                for q in range(2):
                    half[m, i, p, q] = done[q * virt : (q + 1) * virt, p * virt : (p + 1) * virt]

    def push_half(i, register):
        for m in range(UNITS):
            tile = jnp.concatenate(
                [
                    jnp.concatenate([half[m, i, p, q] for q in range(2)], axis=1)
                    for p in range(CHUNK)
                ],
                axis=0,
            )
            pltpu.matmul_push_rhs(tile, staging_register=register, mxu_index=m, transpose=True)

    def second_half(step, i, register):
        turn = step // groups
        for m in range(UNITS):
            q = aux_at(step, m, i)
            pltpu.matmul_acc_lhs(
                ladder_acc[m][turn % 2],
                jnp.concatenate([fact[q], fact[q + 1]], axis=1),
                load_staged_rhs=register,
            )

    def group(step, now, push=None, add=None):
        free = 1 - now
        more = step + 1 < count
        turn_half(0, free)
        if more:
            first_half(step + 1, 0, now)
        push_half(0, free)
        turn_half(1, now)
        if more:
            first_half(step + 1, 1, now)
        push_half(1, now)
        second_half(step, 0, free)
        if push is not None:
            push(free)
            second_half(step, 1, now)
            if step + 2 < count:
                push_amp(step + 2, now)
            add(free)
            return now
        if step + 2 < count:
            push_amp(step + 2, free)
        second_half(step, 1, now)
        return free

    def give(turn):
        total = pltpu.matmul_pop(ladder_acc[0][turn % 2])
        side = pltpu.matmul_pop(left_acc[0])
        for m in range(1, UNITS):
            total = total + pltpu.matmul_pop(ladder_acc[m][turn % 2])
            side = side + pltpu.matmul_pop(left_acc[m])
        for i in range(CHUNK):
            cols = slice(i * virt, (i + 1) * virt)
            value = total[:, cols].T + side[:, cols]
            for k in range(blocks):
                piece = value[k * rows : (k + 1) * rows]
                part[turn, k, i] = piece
                if turn == turns - 1:
                    part_low[k, i] = piece.astype(BF16)
        return scatter(turn)

    norm_sums = [jnp.zeros((8, virt), F32) for _ in range(PASSES)]
    energy = [jnp.zeros((8, virt), F32)]

    def fold(value):
        return jnp.sum(value.reshape(rows // 8, 8, virt), axis=0)

    def finish(turn):
        sweep, start = place(turn)
        last = turn == turns - 1
        for i in range(CHUNK):
            p = start + i
            residual = base[sweep, p] + part[turn, me, i]
            for j in range(blocks - 1):
                residual = residual + (recv_low[j, i].astype(F32) if last else recv[turn, j, i])
            norm_sums[sweep] += fold(residual * residual)
            if last:
                continue
            value = amp[sweep, p] + residual * recip[p]
            amp[sweep + 1, p] = value
            if sweep + 1 < PASSES:
                low[sweep + 1, me, p] = value.astype(BF16)
            elif p < core:
                new_ref[:, border + p, :] = value
                energy[0] = energy[0] + weights[border + p] * fold(value * exch[p])
        if sweep + 1 < PASSES:
            gathers[turn + chunks] = gather(turn + chunks)
            add_hole(sweep + 1, range(start, start + CHUNK), start == 0)

    exports = []

    def export():
        weight_copy.wait_recv()
        for side, target in ((0, sides[1]), (1, sides[0])):
            used = frag < frags - 1 if side == 0 else frag > 0
            for r in range(border):
                value = amp[PASSES, jnp.maximum(export_ref[0, side, r] - border, 0)]
                sent_rows[side, r] = value
                energy[0] = energy[0] + jnp.where(used, fold(value * got_weights[side, r]), 0.0)
            pltpu.make_async_remote_copy(
                src_ref=sent_rows.at[side],
                dst_ref=got_rows.at[side],
                send_sem=ex_send,
                recv_sem=ex_recv,
                device_id={"frag": target},
                device_id_type=MESH,
            ).start()
        exports.append(joint(got_rows, ex_send, ex_recv))
        pending.extend(exports)

    push_amp(0, 1)
    first_half(0, 0, 1)
    first_half(0, 1, 1)
    push_amp(1, 0)
    given = {}
    ring_turn = turns - 1 - pl.cdiv(rounds, every)
    now = 0
    for turn in range(turns):
        for g in range(groups):
            step = turn * groups + g
            lead = GIVE if turn < turns - 1 else LAST_GIVE
            if g == FINISH and turn >= 2:
                given[turn - 2].wait_recv()
            if g == lead + 1:
                now = group(step, now, functools.partial(push_left, turn), add_left)
            elif g == FINISH + 1 and turn - 2 == chunks - 1:
                now = group(step, now, push_fock, functools.partial(add_right, 1))
                take_right(1)
            else:
                now = group(step, now)
            if g == lead:
                if turn > 0:
                    given[turn - 1] = give(turn - 1)
                if ring_turn <= turn < turns - 1:
                    at = (turn - ring_turn) * every
                    for r in range(at, min(at + every, rounds)):
                        ring_wait()
                        if r + 1 < rounds:
                            ring_signal()
            if g == FINISH and turn >= 2:
                finish(turn - 2)
                if turn - 2 == (PASSES - 1) * chunks + core_chunks - 1:
                    export()
    given[turns - 1] = give(turns - 1)
    given[turns - 2].wait_recv()
    finish(turns - 2)
    ends = (frag == 0) | swap
    for i in range(border):
        scale = weight_ref[0, where[core + i]].astype(F32) * 0.5
        product = scale * fold(amp[PASSES, core + i] * exch[core + i])
        energy[0] = energy[0] + jnp.where(ends, product, 0.0)

    def whole(value):
        return jnp.sum(jnp.sum(value, axis=0, keepdims=True), axis=1, keepdims=True)

    lane = lax.broadcasted_iota(jnp.int32, (1, virt), 1)
    sums[device] = jnp.where(lane == 0, whole(energy[0]), 0.0)
    blk_at = [lax.rem(me + j, blocks) for j in range(blocks)]

    def send_sum(i, j):
        pltpu.make_async_remote_copy(
            src_ref=sums.at[device],
            dst_ref=sums.at[device],
            send_sem=sum_send,
            recv_sem=sum_recv,
            device_id={"frag": lax.rem(frag + i, frags), "blk": blk_at[j]},
            device_id_type=MESH,
        ).start()

    def send_sums(i, carry):
        for j in range(blocks):
            send_sum(i, j)
        return carry

    lax.fori_loop(1, frags, send_sums, 0)
    for j in range(1, blocks):
        send_sum(0, j)
    sum_copy = joint(sums.at[pl.ds(0, blocks * frags - 1)], sum_send, sum_recv)
    given[turns - 1].wait_recv()
    finish(turns - 1)
    line = jnp.zeros((1, virt), F32)
    for s in range(PASSES):
        line = jnp.where(lane == s, whole(norm_sums[s]), line)
    squares[me] = line
    for peer in peers:
        pltpu.make_async_remote_copy(
            src_ref=squares.at[me],
            dst_ref=squares.at[me],
            send_sem=sq_send,
            recv_sem=sq_recv,
            device_id={"blk": peer},
            device_id_type=MESH,
        ).start()
    square_copy = joint(squares.at[pl.ds(0, blocks - 1)], sq_send, sq_recv)
    for copy in exports:
        copy.wait_recv()
    for i in range(border):
        value = amp[PASSES, core + i]
        new_ref[:, i, :] = jnp.where(frag > 0, got_rows[0, i], value)
        new_ref[:, pairs - border + i, :] = jnp.where(swap, value, got_rows[1, i])
    for copy in pending:
        copy.wait_send()
    sum_copy.wait_send()
    square_copy.wait_recv()
    roots = jnp.sqrt(jnp.sum(squares[...], axis=0))
    sum_copy.wait_recv()
    total = jnp.sum(sums[...], axis=0)
    scaled = -jnp.sum(total, axis=1, keepdims=True) / (virt * virt)
    line_ref[...] = jnp.where(lane == PASSES, scaled, roots)
    square_copy.wait_send()


def hand_out(new_ref, line_ref, new_out, norm_out, energy_out, norm, energy, sem):
    first = pltpu.make_async_copy(new_ref, new_out, sem.at[0])
    first.start()
    norm[...] = line_ref[:, :PASSES]
    energy[...] = line_ref[:, PASSES : PASSES + 1]
    copies = [
        pltpu.make_async_copy(norm, norm_out, sem.at[1]),
        pltpu.make_async_copy(energy, energy_out, sem.at[2]),
    ]
    for copy in copies:
        copy.start()
    for copy in [first] + copies:
        copy.wait()


def on_device(blocks, frags, *args):
    amps, _, factors = args[:3]
    _, rows, pairs, virt = amps.shape
    aux = factors.shape[1]
    border = args[-1].shape[2]
    turns = PASSES * (pairs // CHUNK)
    vmem = pl.BlockSpec(memory_space=pltpu.VMEM)
    hbm = pl.BlockSpec(memory_space=pltpu.HBM)
    dma = pltpu.SemaphoreType.DMA
    new_amps, line = pl.pallas_call(
        functools.partial(kernel, blocks, frags),
        out_shape=(
            jax.ShapeDtypeStruct(amps.shape[1:], F32),
            jax.ShapeDtypeStruct((1, virt), F32),
        ),
        in_specs=[hbm] * 9,
        out_specs=(vmem, vmem),
        scratch_shapes=[
            pltpu.VMEM((aux, virt, virt), BF16),
            pltpu.VMEM((rows, pairs, virt), F32),
            pltpu.VMEM((rows, pairs, virt), F32),
            pltpu.VMEM((virt, virt), F32),
            pltpu.VMEM((1, virt), F32),
            pltpu.SMEM((1, pairs, pairs), F32),
            pltpu.SMEM((1, pairs), F32),
            pltpu.SMEM((1, pairs), jnp.int32),
            pltpu.SMEM((1, 2, border), jnp.int32),
            pltpu.VMEM((PASSES + 1, pairs, rows, virt), F32),
            pltpu.VMEM((PASSES, blocks, pairs, rows, virt), BF16),
            pltpu.VMEM((UNITS, 2, CHUNK, 2, virt, virt), BF16),
            pltpu.VMEM((turns, blocks, CHUNK, rows, virt), F32),
            pltpu.VMEM((turns, blocks - 1, CHUNK, rows, virt), F32),
            pltpu.VMEM((blocks, CHUNK, rows, virt), BF16),
            pltpu.VMEM((blocks - 1, CHUNK, rows, virt), BF16),
            pltpu.VMEM((pairs, rows, virt), F32),
            pltpu.VMEM((PASSES, pairs, rows, virt), F32),
            pltpu.VMEM((pairs, rows, virt), F32),
            pltpu.VMEM((virt, 2 * virt), BF16),
            pltpu.VMEM((virt, 2 * virt), BF16),
            pltpu.VMEM((rows, virt), F32),
            pltpu.VMEM((virt, virt), F32),
            pltpu.VMEM((2, border, rows, virt), F32),
            pltpu.VMEM((2, border, rows, virt), F32),
            pltpu.VMEM((2, border, rows, virt), F32),
            pltpu.VMEM((2, border, rows, virt), F32),
            pltpu.VMEM((blocks * frags, 1, virt), F32),
            pltpu.VMEM((blocks, 1, virt), F32),
        ],
        compiler_params=pltpu.CompilerParams(
            collective_id=0,
            has_side_effects=True,
            vmem_limit_bytes=48 * 2**20,
        ),
    )(*[pltpu.with_memory_space_constraint(x, pltpu.HBM) for x in args])
    shapes = (new_amps.shape, (1, PASSES), (1, 1))
    new_amps, norms, energy = pl.pallas_call(
        hand_out,
        out_shape=tuple(jax.ShapeDtypeStruct(shape, F32) for shape in shapes),
        in_specs=[vmem] * 2,
        out_specs=(pl.BlockSpec(memory_space=pl.ANY),) * 3,
        scratch_shapes=[pltpu.VMEM(shape, F32) for shape in shapes[1:]] + [dma((3,))],
        compiler_params=pltpu.CompilerParams(vmem_limit_bytes=2**20),
    )(new_amps, line)
    return new_amps.reshape(amps.shape), norms, energy.reshape(())


def solution(mesh):
    placed = (
        P("frag", "blk", None, None),
        P("frag", "blk", None, None),
        P("frag", "blk", None, None),
        P("frag", None, None),
        P("frag", None, None),
        P("frag", None),
        P("frag", None),
        P("frag", None),
        P("frag", None, None),
    )
    return jax.shard_map(
        functools.partial(on_device, mesh.shape["blk"], mesh.shape["frag"]),
        mesh=mesh,
        in_specs=placed,
        out_specs=(P("frag", "blk", None, None), P("frag", None), P()),
        check_vma=False,
    )
```

```python
import functools

import jax
import jax.numpy as jnp
from jax import lax
from jax.experimental import pallas as pl
from jax.experimental.pallas import tpu as pltpu
from jax.sharding import PartitionSpec as P

PASSES = 2
CHUNK = 2
UNITS = 2
GROUP = 8
GIVE = 1
LAST_GIVE = 0
FINISH = 6
MESH = pl.DeviceIdType.MESH
F32, BF16 = jnp.float32, jnp.bfloat16


def halves(value):
    high = value.astype(BF16)
    return high, (value - high.astype(F32)).astype(BF16)


def kernel(blocks, frags, *refs):
    virt = refs[0].shape[3]
    tall, flat = (2 * virt, 2 * virt), (virt, 2 * virt)

    turns = PASSES * (refs[0].shape[2] // CHUNK)
    dma = pltpu.SemaphoreType.DMA

    def body(first, ladder, left, right, semaphores):
        run(blocks, frags, first, ladder, left, right, *refs, *semaphores)

    pl.run_scoped(
        body,
        [[pltpu.ACC(m)(tall, F32) for _ in range(2)] for m in range(UNITS)],
        [[pltpu.ACC(m)(flat, F32) for _ in range(2)] for m in range(UNITS)],
        [pltpu.ACC(m)(flat, F32) for m in range(UNITS)],
        [pltpu.ACC(m)(flat, F32) for m in range(UNITS)],
        [pltpu.SemaphoreType.REGULAR((2,)), dma((8,)), dma] + [dma((turns,))] * 4 + [dma] * 8,
    )


def run(
    blocks,
    frags,
    first_acc,
    ladder_acc,
    left_acc,
    right_acc,
    amps_hbm,
    exch_hbm,
    factors_hbm,
    hole_hbm,
    fock_hbm,
    orbital_hbm,
    pair_hbm,
    weight_hbm,
    export_hbm,
    new_ref,
    line_ref,
    fact,
    amps_in,
    exch_in,
    fock_in,
    orbital_in,
    hole_ref,
    pair_ref,
    weight_ref,
    export_ref,
    amp,
    low,
    half,
    part,
    recv,
    part_low,
    recv_low,
    exch,
    base,
    recip,
    fock_row,
    fock_col,
    row_energy,
    row_t,
    sent_rows,
    got_rows,
    sent_weights,
    got_weights,
    sums,
    squares,
    ring,
    in_sem,
    fact_sem,
    ag_send,
    ag_recv,
    rs_send,
    rs_recv,
    ex_send,
    ex_recv,
    we_send,
    we_recv,
    sum_send,
    sum_recv,
    sq_send,
    sq_recv,
):
    me = lax.axis_index("blk")
    frag = lax.axis_index("frag")
    rows, pairs, virt = amps_in.shape
    aux = fact.shape[0]
    groups = aux // GROUP
    border = export_hbm.shape[2]
    device = frag * blocks + me
    peers = [lax.rem(me + j, blocks) for j in range(1, blocks)]
    core = pairs - 2 * border
    swap = frag == frags - 1

    def pair_at(place):
        if place < core:
            return border + place
        at = (place - core) % border
        lower, upper = at, pairs - border + at
        if place - core < border:
            return jnp.where(swap, upper, lower)
        return jnp.where(swap, lower, upper)

    def take(ref, place):
        if place < core:
            return ref[:, border + place, :]
        at = (place - core) % border
        lower, upper = ref[:, at, :], ref[:, pairs - border + at, :]
        if place - core < border:
            return jnp.where(swap, upper, lower)
        return jnp.where(swap, lower, upper)

    chunks = pairs // CHUNK
    core_chunks = core // CHUNK
    turns = PASSES * chunks
    count = turns * groups

    def place(turn):
        return turn // chunks, turn % chunks * CHUNK

    sides = [lax.rem(frag + frags - 1, frags), lax.rem(frag + 1, frags)]

    def joint(ref, send_sem, recv_sem):
        return pltpu.make_async_remote_copy(
            src_ref=ref,
            dst_ref=ref,
            send_sem=send_sem,
            recv_sem=recv_sem,
            device_id={"blk": peers[0]},
            device_id_type=MESH,
        )

    loads = []
    for i, (src, dst) in enumerate(
        (
            (amps_hbm.at[0], amps_in),
            (fock_hbm.at[0], fock_in),
            (orbital_hbm, orbital_in),
            (pair_hbm, pair_ref),
            (hole_hbm, hole_ref),
            (exch_hbm.at[0], exch_in),
            (weight_hbm, weight_ref),
            (export_hbm, export_ref),
        )
    ):
        loads.append(pltpu.make_async_copy(src, dst, in_sem.at[i]))
    fact_load = pltpu.make_async_copy(factors_hbm.at[0], fact, fact_sem)
    barrier = pltpu.get_barrier_semaphore()
    loads[0].start()
    for side in sides:
        pl.semaphore_signal(barrier, inc=1, device_id={"frag": side}, device_id_type=MESH)
    for peer in peers:
        pl.semaphore_signal(barrier, inc=1, device_id={"blk": peer}, device_id_type=MESH)
    for copy in loads[1:]:
        copy.start()
    fact_load.start()

    rounds = frags // 2
    slots = range(2, 2 * turns - 2, 3)
    every = pl.cdiv(rounds, len(slots))

    def ring_signal():
        for i, side in enumerate(sides):
            pl.semaphore_signal(
                ring.at[i], inc=1, device_id={"frag": side}, device_id_type=MESH
            )

    def ring_wait():
        for i in range(2):
            pl.semaphore_wait(ring.at[i], 1)

    for m in range(UNITS):
        for ref in first_acc[m] + ladder_acc[m] + [left_acc[m], right_acc[m]]:
            pltpu.matmul_pop(ref)

    loads[0].wait()

    def enter(place):
        value = take(amps_in, place)
        amp[0, place] = value
        low[0, me, place] = value.astype(BF16)

    for place_at in range(CHUNK):
        enter(place_at)
    pl.semaphore_wait(barrier, blocks - 1 + 2)

    pending = []

    def gather(turn):
        sweep, start = place(turn)
        where = low.at[sweep, me, pl.ds(start, CHUNK)]
        for peer in peers:
            pltpu.make_async_remote_copy(
                src_ref=where,
                dst_ref=where,
                send_sem=ag_send.at[turn],
                recv_sem=ag_recv.at[turn],
                device_id={"blk": peer},
                device_id_type=MESH,
            ).start()
        span = low.at[sweep, pl.ds(0, blocks - 1), pl.ds(start, CHUNK)]
        pending.append(joint(span, ag_send.at[turn], ag_recv.at[turn]))
        return pending[-1]

    gathers = {0: gather(0)}
    for turn in range(1, chunks):
        for i in range(CHUNK):
            enter(turn * CHUNK + i)
        gathers[turn] = gather(turn)

    def scatter(turn):
        last = turn == turns - 1
        source, target = (part_low, recv_low) if last else (part.at[turn], recv.at[turn])
        for j, peer in enumerate(peers):
            pltpu.make_async_remote_copy(
                src_ref=source.at[peer],
                dst_ref=target.at[j],
                send_sem=rs_send.at[turn],
                recv_sem=rs_recv.at[turn],
                device_id={"blk": peer},
                device_id_type=MESH,
            ).start()
        pending.append(joint(target, rs_send.at[turn], rs_recv.at[turn]))
        return pending[-1]

    offset = pl.multiple_of(me * rows, rows)
    for copy in loads[1:5]:
        copy.wait()
    column = lax.broadcasted_iota(jnp.int32, (virt, virt), 1)
    own = (column >= offset) & (column < offset + rows)
    high, middle = halves(fock_in[...])
    fock_row[:, :virt] = high
    fock_row[:, virt:] = middle
    high, middle = halves(jnp.where(own, fock_in[...], 0.0))
    fock_col[:, :virt] = high
    fock_col[:, virt:] = middle
    row_t[...] = jnp.broadcast_to(orbital_in[...], (virt, virt)).T
    row_energy[...] = row_t[pl.ds(offset, rows), :] + orbital_in[...]
    where = [pair_at(p) for p in range(pairs)]
    levels = [pair_ref[0, p] for p in where]
    for p in range(pairs):
        recip[p] = 1.0 / (row_energy[...] - levels[p])
    for copy in loads[5:]:
        copy.wait()
    weights = [weight_ref[0, p].astype(F32) * 0.5 for p in range(pairs)]
    for p in range(pairs):
        exch[p] = take(exch_in, p)
    for i, side in enumerate(sides):
        for r in range(border):
            p = r if i == 0 else pairs - border + r
            sent_weights[i, r] = exch_in[:, p, :] * weights[p]
    for i, side in enumerate(sides):
        pltpu.make_async_remote_copy(
            src_ref=sent_weights.at[i],
            dst_ref=got_weights.at[i],
            send_sem=we_send,
            recv_sem=we_recv,
            device_id={"frag": side},
            device_id_type=MESH,
        ).start()
    weight_copy = joint(got_weights, we_send, we_recv)
    pending.append(weight_copy)
    ring_signal()

    def add_hole(sweep, places, fresh):
        for p in range(pairs):
            total = exch[p] if fresh else base[sweep, p]
            for r in places:
                total = total + hole_ref[0, where[p], where[r]] * amp[sweep, r]
                if r == p:
                    total = total - (row_energy[...] - levels[p]) * amp[sweep, p]
            base[sweep, p] = total

    share = pairs // UNITS

    def push_fock(register):
        tile = jnp.concatenate([fock_row[...], jnp.zeros((virt, 2 * virt), BF16)], axis=0)
        for m in range(UNITS):
            pltpu.matmul_push_rhs(tile, staging_register=register, mxu_index=m, transpose=True)

    def add_right(sweep, register):
        for m in range(UNITS):
            split = halves(amp[sweep, m * share : (m + 1) * share].reshape(share * rows, virt))
            for i, value in enumerate(split):
                pltpu.matmul_acc_lhs(
                    right_acc[m],
                    jnp.concatenate([value, value], axis=1),
                    load_staged_rhs=register if i == 0 else None,
                )

    def take_right(sweep):
        for m in range(UNITS):
            product = pltpu.matmul_pop(right_acc[m])
            for k in range(share):
                p = m * share + k
                base[sweep, p] += product[k * rows : (k + 1) * rows, :virt]

    push_fock(0)
    add_right(0, 0)
    add_hole(0, range(pairs), True)
    take_right(0)

    def push_left(turn, register):
        sweep, start = place(turn)
        split = [halves(amp[sweep, start + i]) for i in range(CHUNK)]
        for m in range(UNITS):
            tile = jnp.concatenate([split[i][m] for i in range(CHUNK)], axis=1)
            tile = jnp.concatenate([tile] * (2 * blocks), axis=0)
            pltpu.matmul_push_rhs(tile, staging_register=register, mxu_index=m)

    def add_left(register):
        for m in range(UNITS):
            pltpu.matmul_acc_lhs(left_acc[m], fock_col[...], load_staged_rhs=register)

    def aux_at(step, m, i):
        return (step % groups) * GROUP + m * (GROUP // UNITS) + 2 * i

    def push_amp(step, register):
        turn = step // groups
        sweep, start = place(turn)
        if step % groups == 0:
            gathers[turn].wait_recv()
        tile = jnp.concatenate(
            [low[sweep, :, start + i].reshape(virt, virt) for i in range(CHUNK)], axis=1
        )
        tile = jnp.concatenate([tile, jnp.zeros((virt, 2 * virt), BF16)], axis=0)
        for m in range(UNITS):
            pltpu.matmul_push_rhs(tile, staging_register=register, mxu_index=m)

    def first_half(step, i, register):
        if step == 0 and i == 0:
            fact_load.wait()
        for m in range(UNITS):
            q = aux_at(step, m, i)
            slab = fact[q : q + 2].reshape(2 * virt, virt)
            pltpu.matmul_acc_lhs(
                first_acc[m][i],
                jnp.concatenate([slab, jnp.zeros_like(slab)], axis=1),
                load_staged_rhs=register if i == 0 else None,
            )

    def turn_half(i, register):
        for m in range(UNITS):
            done = pltpu.matmul_pop(first_acc[m][i]).astype(BF16)
            for p in range(CHUNK):
                for q in range(2):
                    half[m, i, p, q] = done[q * virt : (q + 1) * virt, p * virt : (p + 1) * virt]

    def push_half(i, register):
        for m in range(UNITS):
            tile = jnp.concatenate(
                [
                    jnp.concatenate([half[m, i, p, q] for q in range(2)], axis=1)
                    for p in range(CHUNK)
                ],
                axis=0,
            )
            pltpu.matmul_push_rhs(tile, staging_register=register, mxu_index=m, transpose=True)

    def second_half(step, i, register):
        turn = step // groups
        for m in range(UNITS):
            q = aux_at(step, m, i)
            pltpu.matmul_acc_lhs(
                ladder_acc[m][turn % 2],
                jnp.concatenate([fact[q], fact[q + 1]], axis=1),
                load_staged_rhs=register,
            )

    def group(step, now, push=None, add=None):
        free = 1 - now
        more = step + 1 < count
        turn_half(0, free)
        if more:
            first_half(step + 1, 0, now)
        push_half(0, free)
        turn_half(1, now)
        if more:
            first_half(step + 1, 1, now)
        push_half(1, now)
        second_half(step, 0, free)
        if push is not None:
            push(free)
            second_half(step, 1, now)
            if step + 2 < count:
                push_amp(step + 2, now)
            add(free)
            return now
        if step + 2 < count:
            push_amp(step + 2, free)
        second_half(step, 1, now)
        return free

    def give(turn):
        total = pltpu.matmul_pop(ladder_acc[0][turn % 2])
        side = pltpu.matmul_pop(left_acc[0])
        for m in range(1, UNITS):
            total = total + pltpu.matmul_pop(ladder_acc[m][turn % 2])
            side = side + pltpu.matmul_pop(left_acc[m])
        for i in range(CHUNK):
            cols = slice(i * virt, (i + 1) * virt)
            value = total[:, cols].T + side[:, cols]
            for k in range(blocks):
                piece = value[k * rows : (k + 1) * rows]
                part[turn, k, i] = piece
                if turn == turns - 1:
                    part_low[k, i] = piece.astype(BF16)
        return scatter(turn)

    norm_sums = [jnp.zeros((8, virt), F32) for _ in range(PASSES)]
    energy = [jnp.zeros((8, virt), F32)]

    def fold(value):
        return jnp.sum(value.reshape(rows // 8, 8, virt), axis=0)

    def finish(turn):
        sweep, start = place(turn)
        last = turn == turns - 1
        for i in range(CHUNK):
            p = start + i
            residual = base[sweep, p] + part[turn, me, i]
            for j in range(blocks - 1):
                residual = residual + (recv_low[j, i].astype(F32) if last else recv[turn, j, i])
            norm_sums[sweep] += fold(residual * residual)
            if last:
                continue
            value = amp[sweep, p] + residual * recip[p]
            amp[sweep + 1, p] = value
            if sweep + 1 < PASSES:
                low[sweep + 1, me, p] = value.astype(BF16)
            elif p < core:
                new_ref[:, border + p, :] = value
                energy[0] = energy[0] + weights[border + p] * fold(value * exch[p])
        if sweep + 1 < PASSES:
            gathers[turn + chunks] = gather(turn + chunks)
            add_hole(sweep + 1, range(start, start + CHUNK), start == 0)

    exports = []

    def export():
        weight_copy.wait_recv()
        for side, target in ((0, sides[1]), (1, sides[0])):
            used = frag < frags - 1 if side == 0 else frag > 0
            for r in range(border):
                value = amp[PASSES, jnp.maximum(export_ref[0, side, r] - border, 0)]
                sent_rows[side, r] = value
                energy[0] = energy[0] + jnp.where(used, fold(value * got_weights[side, r]), 0.0)
            pltpu.make_async_remote_copy(
                src_ref=sent_rows.at[side],
                dst_ref=got_rows.at[side],
                send_sem=ex_send,
                recv_sem=ex_recv,
                device_id={"frag": target},
                device_id_type=MESH,
            ).start()
        exports.append(joint(got_rows, ex_send, ex_recv))
        pending.extend(exports)

    push_amp(0, 1)
    first_half(0, 0, 1)
    first_half(0, 1, 1)
    push_amp(1, 0)
    given = {}
    def ring_step(slot):
        if slot in slots:
            at = slots.index(slot) * every
            for r in range(at, min(at + every, rounds)):
                ring_wait()
                if r + 1 < rounds:
                    ring_signal()

    now = 0
    for turn in range(turns):
        for g in range(groups):
            step = turn * groups + g
            lead = GIVE if turn < turns - 1 else LAST_GIVE
            if g == FINISH and turn >= 2:
                given[turn - 2].wait_recv()
            if g == lead + 1:
                now = group(step, now, functools.partial(push_left, turn), add_left)
            elif g == FINISH + 1 and turn - 2 == chunks - 1:
                now = group(step, now, push_fock, functools.partial(add_right, 1))
                take_right(1)
            else:
                now = group(step, now)
            if g == lead:
                if turn > 0:
                    given[turn - 1] = give(turn - 1)
                ring_step(2 * turn)
            if g == FINISH and turn >= 2:
                finish(turn - 2)
                if turn - 2 == (PASSES - 1) * chunks + core_chunks - 1:
                    export()
            if g == FINISH:
                ring_step(2 * turn + 1)
    given[turns - 1] = give(turns - 1)
    given[turns - 2].wait_recv()
    finish(turns - 2)
    ends = (frag == 0) | swap
    for i in range(border):
        scale = weight_ref[0, where[core + i]].astype(F32) * 0.5
        product = scale * fold(amp[PASSES, core + i] * exch[core + i])
        energy[0] = energy[0] + jnp.where(ends, product, 0.0)

    def whole(value):
        return jnp.sum(jnp.sum(value, axis=0, keepdims=True), axis=1, keepdims=True)

    lane = lax.broadcasted_iota(jnp.int32, (1, virt), 1)
    sums[device] = jnp.where(lane == 0, whole(energy[0]), 0.0)
    blk_at = [lax.rem(me + j, blocks) for j in range(blocks)]

    def send_sum(i, j):
        pltpu.make_async_remote_copy(
            src_ref=sums.at[device],
            dst_ref=sums.at[device],
            send_sem=sum_send,
            recv_sem=sum_recv,
            device_id={"frag": lax.rem(frag + i, frags), "blk": blk_at[j]},
            device_id_type=MESH,
        ).start()

    def send_sums(i, carry):
        for j in range(blocks):
            send_sum(i, j)
        return carry

    lax.fori_loop(1, frags, send_sums, 0)
    for j in range(1, blocks):
        send_sum(0, j)
    sum_copy = joint(sums.at[pl.ds(0, blocks * frags - 1)], sum_send, sum_recv)
    given[turns - 1].wait_recv()
    finish(turns - 1)
    line = jnp.zeros((1, virt), F32)
    for s in range(PASSES):
        line = jnp.where(lane == s, whole(norm_sums[s]), line)
    squares[me] = line
    for peer in peers:
        pltpu.make_async_remote_copy(
            src_ref=squares.at[me],
            dst_ref=squares.at[me],
            send_sem=sq_send,
            recv_sem=sq_recv,
            device_id={"blk": peer},
            device_id_type=MESH,
        ).start()
    square_copy = joint(squares.at[pl.ds(0, blocks - 1)], sq_send, sq_recv)
    for copy in exports:
        copy.wait_recv()
    for i in range(border):
        value = amp[PASSES, core + i]
        new_ref[:, i, :] = jnp.where(frag > 0, got_rows[0, i], value)
        new_ref[:, pairs - border + i, :] = jnp.where(swap, value, got_rows[1, i])
    for copy in pending:
        copy.wait_send()
    sum_copy.wait_send()
    square_copy.wait_recv()
    roots = jnp.sqrt(jnp.sum(squares[...], axis=0))
    sum_copy.wait_recv()
    total = jnp.sum(sums[...], axis=0)
    scaled = -jnp.sum(total, axis=1, keepdims=True) / (virt * virt)
    line_ref[...] = jnp.where(lane == PASSES, scaled, roots)
    square_copy.wait_send()


def hand_out(new_ref, line_ref, new_out, norm_out, energy_out, norm, energy, sem):
    first = pltpu.make_async_copy(new_ref, new_out, sem.at[0])
    first.start()
    norm[...] = line_ref[:, :PASSES]
    energy[...] = line_ref[:, PASSES : PASSES + 1]
    copies = [
        pltpu.make_async_copy(norm, norm_out, sem.at[1]),
        pltpu.make_async_copy(energy, energy_out, sem.at[2]),
    ]
    for copy in copies:
        copy.start()
    for copy in [first] + copies:
        copy.wait()


def on_device(blocks, frags, *args):
    amps, _, factors = args[:3]
    _, rows, pairs, virt = amps.shape
    aux = factors.shape[1]
    border = args[-1].shape[2]
    turns = PASSES * (pairs // CHUNK)
    vmem = pl.BlockSpec(memory_space=pltpu.VMEM)
    hbm = pl.BlockSpec(memory_space=pltpu.HBM)
    dma = pltpu.SemaphoreType.DMA
    new_amps, line = pl.pallas_call(
        functools.partial(kernel, blocks, frags),
        out_shape=(
            jax.ShapeDtypeStruct(amps.shape[1:], F32),
            jax.ShapeDtypeStruct((1, virt), F32),
        ),
        in_specs=[hbm] * 9,
        out_specs=(vmem, vmem),
        scratch_shapes=[
            pltpu.VMEM((aux, virt, virt), BF16),
            pltpu.VMEM((rows, pairs, virt), F32),
            pltpu.VMEM((rows, pairs, virt), F32),
            pltpu.VMEM((virt, virt), F32),
            pltpu.VMEM((1, virt), F32),
            pltpu.SMEM((1, pairs, pairs), F32),
            pltpu.SMEM((1, pairs), F32),
            pltpu.SMEM((1, pairs), jnp.int32),
            pltpu.SMEM((1, 2, border), jnp.int32),
            pltpu.VMEM((PASSES + 1, pairs, rows, virt), F32),
            pltpu.VMEM((PASSES, blocks, pairs, rows, virt), BF16),
            pltpu.VMEM((UNITS, 2, CHUNK, 2, virt, virt), BF16),
            pltpu.VMEM((turns, blocks, CHUNK, rows, virt), F32),
            pltpu.VMEM((turns, blocks - 1, CHUNK, rows, virt), F32),
            pltpu.VMEM((blocks, CHUNK, rows, virt), BF16),
            pltpu.VMEM((blocks - 1, CHUNK, rows, virt), BF16),
            pltpu.VMEM((pairs, rows, virt), F32),
            pltpu.VMEM((PASSES, pairs, rows, virt), F32),
            pltpu.VMEM((pairs, rows, virt), F32),
            pltpu.VMEM((virt, 2 * virt), BF16),
            pltpu.VMEM((virt, 2 * virt), BF16),
            pltpu.VMEM((rows, virt), F32),
            pltpu.VMEM((virt, virt), F32),
            pltpu.VMEM((2, border, rows, virt), F32),
            pltpu.VMEM((2, border, rows, virt), F32),
            pltpu.VMEM((2, border, rows, virt), F32),
            pltpu.VMEM((2, border, rows, virt), F32),
            pltpu.VMEM((blocks * frags, 1, virt), F32),
            pltpu.VMEM((blocks, 1, virt), F32),
        ],
        compiler_params=pltpu.CompilerParams(
            collective_id=0,
            has_side_effects=True,
            vmem_limit_bytes=48 * 2**20,
        ),
    )(*[pltpu.with_memory_space_constraint(x, pltpu.HBM) for x in args])
    shapes = (new_amps.shape, (1, PASSES), (1, 1))
    new_amps, norms, energy = pl.pallas_call(
        hand_out,
        out_shape=tuple(jax.ShapeDtypeStruct(shape, F32) for shape in shapes),
        in_specs=[vmem] * 2,
        out_specs=(pl.BlockSpec(memory_space=pl.ANY),) * 3,
        scratch_shapes=[pltpu.VMEM(shape, F32) for shape in shapes[1:]] + [dma((3,))],
        compiler_params=pltpu.CompilerParams(vmem_limit_bytes=2**20),
    )(new_amps, line)
    return new_amps.reshape(amps.shape), norms, energy.reshape(())


def solution(mesh):
    placed = (
        P("frag", "blk", None, None),
        P("frag", "blk", None, None),
        P("frag", "blk", None, None),
        P("frag", None, None),
        P("frag", None, None),
        P("frag", None),
        P("frag", None),
        P("frag", None),
        P("frag", None, None),
    )
    return jax.shard_map(
        functools.partial(on_device, mesh.shape["blk"], mesh.shape["frag"]),
        mesh=mesh,
        in_specs=placed,
        out_specs=(P("frag", "blk", None, None), P("frag", None), P()),
        check_vma=False,
    )
```
